128 devices in a mesh: groups: 4 (over x, y), blk: 32 (over z, core).
Axes of the slice: x: 2, y: 2, z: 16, core: 2. Of those that a mesh axis runs over, the one named last changes fastest.
The devices are a block of a 8x8x16 slice.
Arguments:
- coords: float32 [32, 98304], P(None, ('groups', 'blk')), parts along dimension 1, may hold values from -6 to 6
- alpha: float32 [98304], P(('groups', 'blk')), parts along dimension 0, may hold values from -6 to 6
- probe_solves: float32 [15, 98304], P(None, ('groups', 'blk')), parts along dimension 1, may hold values from -6 to 6
- probes: float32 [15, 98304], P(None, ('groups', 'blk')), parts along dimension 1, may hold values from -6 to 6
- lengthscale: float32 [32], replicated, may hold values from 4 to 12
Outputs:
- grad: float32 [32, 98304], P(None, ('groups', 'blk')), parts along dimension 1
The draws below stay inside these ranges and needn't reach their ends.
There are 4 independent parts, one for each index of `groups`. The reference program is written for one: setup_inputs(seed, part) draws one part's arguments, and reference() takes and returns one part's arrays. A program takes and returns all parts, laid end to end along the dimension named above; an argument that names none is the same for every part. Nothing has to cross between parts.
All inputs are finite; a program needn't handle non-finite values.
Results may differ from the reference program's by a relative error of at most 0.00014.
Values sent between devices are 32-bit elements; how exact they have to be, the bound alone decides.
No kernel may reach another device: no remote copies, remote signals or barrier semaphores. Data moves between devices by JAX's collectives and lax.ppermute only.
A program may use at most 64 MiB of HBM per device.

```python
import math
import jax
import jax.numpy as jnp
from jax import lax

DIM = 32
PROBES = 15
BLOCK = 768
STEPS = 8
NPTS = 24576
N_BLK = 32


def levels(own_key, extent, shards, least, largest):
    level, own = 1.0, jax.random.fold_in(own_key, 6)
    for dim, blocks in shards:
        heights = jnp.exp(jax.random.uniform(jax.random.fold_in(own, dim), (blocks,), jnp.float32, least / len(shards), largest / len(shards)))
        level = level * jnp.repeat(heights, extent[dim] // blocks).reshape([-1 if axis == dim else 1 for axis in range(len(extent))])
    return level


def scatter_about(key, dims, deviation, most, split=(), dtype=jnp.bfloat16):
    drawn = deviation * jax.random.normal(key, dims, jnp.float32)
    if split:
        drawn = drawn * levels(key, dims, split, -0.22, 0.18)
    return jnp.clip(drawn, -most, most).astype(dtype)


def setup_inputs(seed: int = 0, part: int = 0) -> dict:
    seeds = jax.random.split(jax.random.key(seed), 6)
    part_splits = jax.random.split(jax.random.fold_in(seeds[5], part), 6)
    return {
        "coords": scatter_about(part_splits[0], (DIM, NPTS), 1.0, 6.0, ((1, 32),), jnp.float32),
        "alpha": scatter_about(part_splits[1], (NPTS,), 1.0, 6.0, ((0, 32),), jnp.float32),
        "probe_solves": scatter_about(part_splits[2], (PROBES, NPTS), 1.0, 6.0, ((1, 32),), jnp.float32),
        "probes": scatter_about(part_splits[3], (PROBES, NPTS), 1.0, 6.0, ((1, 32),), jnp.float32),
        "lengthscale": jnp.clip(jnp.exp(jax.random.uniform(seeds[4], (DIM,), jnp.float32, math.log(4.0), math.log(12.0))), 4.0, 12.0),
    }


root_five = 5.0 ** 0.5

def tile_terms(own_scaled, own_table, vis_scaled, vis_table):
    probe_count = (own_table.shape[0] - 1) // 2
    half_inv = 1.0 / (2.0 * probe_count)
    left_rows = jnp.concatenate([own_table[:1], -half_inv * own_table[1:]], 0)
    right_rows = jnp.concatenate([vis_table[:1], vis_table[1 + probe_count:], vis_table[1:1 + probe_count]], 0)
    contract_first = (((0,), (0,)), ((), ()))
    inner = lax.dot_general(own_scaled, vis_scaled, contract_first, precision=lax.Precision.HIGHEST, preferred_element_type=jnp.float32)
    own_square = lax.optimization_barrier(jnp.sum(own_scaled * own_scaled, 0))
    vis_square = lax.optimization_barrier(jnp.sum(vis_scaled * vis_scaled, 0))
    distance = own_square[:, None] + vis_square[None, :] - 2.0 * inner
    radius = jnp.sqrt(jnp.maximum(distance, 0.0))
    profile = (1.0 + root_five * radius) * jnp.exp(-root_five * radius)
    coupling = lax.dot_general(left_rows, right_rows, contract_first, precision=lax.Precision.HIGHEST, preferred_element_type=jnp.float32)
    weighted = coupling * profile
    row_part = own_scaled * lax.optimization_barrier(jnp.sum(weighted, 1))[None, :] - lax.dot_general(vis_scaled, weighted, (((1,), (1,)), ((), ())), precision=lax.Precision.HIGHEST, preferred_element_type=jnp.float32)
    col_part = vis_scaled * lax.optimization_barrier(jnp.sum(weighted, 0))[None, :] - jnp.dot(own_scaled, weighted, precision=lax.Precision.HIGHEST, preferred_element_type=jnp.float32)
    return (row_part, col_part)

def reference(coords, alpha, probe_solves, probes, lengthscale):
    scaled = coords / lengthscale[:, None]
    table = jnp.concatenate([alpha[None], probe_solves, probes], 0)
    blocks_scaled = scaled.reshape(DIM, N_BLK, BLOCK).transpose(1, 0, 2)
    blocks_table = table.reshape(table.shape[0], N_BLK, BLOCK).transpose(1, 0, 2)
    row_total = jnp.zeros(blocks_scaled.shape, jnp.float32)
    col_total = jnp.zeros(blocks_scaled.shape, jnp.float32)
    for offset in range(1, STEPS + 1):
        vis_scaled = jnp.roll(blocks_scaled, -offset, axis=0)
        vis_table = jnp.roll(blocks_table, -offset, axis=0)
        rows_now, cols_now = lax.map(lambda pieces: tile_terms(pieces[0], pieces[1], pieces[2], pieces[3]), (blocks_scaled, blocks_table, vis_scaled, vis_table))
        row_total = row_total + rows_now
        col_total = col_total + jnp.roll(cols_now, offset, axis=0)
    summed = (row_total + col_total).transpose(1, 0, 2).reshape(DIM, N_BLK * BLOCK)
    return -(5.0 / 3.0) / lengthscale[:, None] * summed
```

```python
import functools

import jax
import jax.numpy as jnp
from jax import lax
from jax.experimental import pallas as pl
from jax.experimental.pallas import tpu as pltpu
from jax.sharding import PartitionSpec as P

root_five = 5.0**0.5
minus_log2e = -1.4426950408889634
f32, bf16 = jnp.float32, jnp.bfloat16
VMEM = pl.BlockSpec(memory_space=pltpu.VMEM)
DIM, GROUP, SUMS = 32, 16, 80
STEP = 256


def halves(value):
    high = value.astype(bf16)
    return high, (value - high.astype(f32)).astype(bf16)


def row_is(row, value, other):
    return jnp.where(lax.broadcasted_iota(jnp.int32, other.shape, 0) == row, value, other)


def edge_rows(square, parts_at, ones_at):
    one = square.astype(bf16).astype(f32)
    rest = square - one
    two = rest.astype(bf16).astype(f32)
    row = lax.broadcasted_iota(jnp.int32, square.shape, 0)
    edge = jnp.where((row >= ones_at) & (row < ones_at + 3), 1.0, 0.0)
    for index, part in enumerate((one, two, rest - two)):
        edge = row_is(parts_at + index, part, edge)
    return edge.astype(bf16)


def own_forms(field, dist_ref, coup_ref):
    high, low = halves(field[:DIM])
    first, second = field[DIM : DIM + GROUP], field[DIM + GROUP :]
    square = jnp.broadcast_to(second[:1], first.shape)
    dist_ref[...] = jnp.concatenate([high, low, high, low, edge_rows(square, 3, 0)], 0)
    table = jnp.concatenate([row_is(0, first, second), row_is(0, 0.0, first)], 0)
    high, low = halves(table)
    coup_ref[...] = jnp.concatenate([high, low, high, low], 0)


def visit_forms(half_inv, field, dist_ref, coup_ref, sums_ref):
    points = field.shape[1]
    high, low = halves(field[:DIM])
    first, second = field[DIM : DIM + GROUP], field[DIM + GROUP :]
    sums_ref[...] = jnp.concatenate([high, low, jnp.ones((GROUP, points), bf16)], 0)
    square = jnp.broadcast_to(second[:1], first.shape)
    twice = [-2.0 * high, -2.0 * low]
    zero = jnp.zeros((256 - 4 * DIM - GROUP, points), bf16)
    dist = jnp.concatenate([*twice, *twice[::-1], edge_rows(square, 0, 3), zero], 0)
    dist_ref[...] = dist.T
    table = jnp.concatenate(
        [row_is(0, first, -half_inv * first), row_is(0, 0.0, -half_inv * second)], 0
    )
    high, low = halves(table)
    coup_ref[...] = jnp.concatenate([high, high, low, low], 0).T


def weights(dist, coup):
    dist = jnp.maximum(dist, 1e-30)
    scaled = dist * lax.rsqrt(dist)
    return coup * ((1.0 + scaled) * jnp.exp2(scaled * minus_log2e))


def dot(left, right):
    return lax.dot_general(
        left, right, (((1,), (0,)), ((), ())), preferred_element_type=f32
    )


def add_tile(vis, own, acc_ref, high_ref, low_ref, slot):
    vis_dist, vis_coup, vis_sums = vis
    own_dist, own_coup = own
    points = acc_ref.shape[1]
    depth = own_dist.shape[0]
    width = high_ref.shape[2]
    for start in range(0, points, width):
        cols = slice(start, start + width)
        for begin in range(0, points, STEP):
            rows = slice(begin, begin + STEP)
            dist = dot(vis_dist[rows, :depth], own_dist[:, cols])
            coup = dot(vis_coup[rows, :], own_coup[:, cols])
            high, low = halves(weights(dist, coup))
            high_ref[slot, rows, :] = high
            low_ref[slot, rows, :] = low
        sums = vis_sums[...]
        acc_ref[:, cols] += dot(sums, high_ref[slot]) + dot(sums, low_ref[slot])
        slot = 1 - slot
    return slot


def finish(field, acc):
    high, low = halves(field[:DIM])
    near = high.astype(f32) + low.astype(f32)
    return near * acc[2 * DIM : 2 * DIM + 1] - (acc[:DIM] + acc[DIM : 2 * DIM])


def visit_kernel(half_inv, pairs, n_vis, n_own, n_acc, n_form, done, *refs):
    refs = list(refs)

    def take(count):
        taken, refs[:] = refs[:count], refs[count:]
        return taken

    vis = take(n_vis)
    own = [take(2) for _ in range(n_own)]
    acc_in = take(n_acc)
    fields = take(len(done))
    acc_out = take(n_own)
    forms = [take(2) for _ in range(n_form)]
    outs = take(len(done))
    high_ref, low_ref = take(2)
    for index in range(n_own):
        if index < n_acc:
            acc_out[index][...] = acc_in[index][...]
        else:
            acc_out[index][...] = jnp.zeros_like(acc_out[index])
    for index in range(n_form):
        own_forms(vis[index][...], *forms[index])
    sides = []
    for ref in vis:
        side = take(3)
        visit_forms(half_inv, ref[...], *side)
        sides.append(side)
    slot = 0
    for v, o in pairs:
        slot = add_tile(sides[v], own[o], acc_out[o], high_ref, low_ref, slot)
    for o, field, out in zip(done, fields, outs):
        out[...] = finish(field[...], acc_out[o][...])


def visit(half_inv, pairs, vis, own, accs, n_form=0, done=(), fields=()):
    points = vis[0].shape[1]
    n_own = len(own)
    acc_shape = jax.ShapeDtypeStruct((SUMS, points), f32)
    form_shapes = [
        jax.ShapeDtypeStruct((4 * DIM + GROUP, points), bf16),
        jax.ShapeDtypeStruct((8 * GROUP, points), bf16),
    ]
    out_shape = [acc_shape] * n_own + form_shapes * n_form
    out_shape += [jax.ShapeDtypeStruct((DIM, points), f32)] * len(done)
    scratch = [pltpu.VMEM((2, points, 256), bf16)] * 2
    for _ in vis:
        scratch += [
            pltpu.VMEM((points, 256), bf16),
            pltpu.VMEM((points, 8 * GROUP), bf16),
            pltpu.VMEM((SUMS, points), bf16),
        ]
    args = [*vis, *[ref for forms in own for ref in forms], *accs, *fields]
    first = len(vis) + 2 * n_own
    return pl.pallas_call(
        functools.partial(
            visit_kernel, half_inv, pairs, len(vis), n_own, len(accs), n_form, done
        ),
        out_shape=out_shape,
        in_specs=[VMEM] * len(args),
        out_specs=[VMEM] * len(out_shape),
        scratch_shapes=scratch,
        input_output_aliases={first + index: index for index in range(len(accs))},
        compiler_params=pltpu.CompilerParams(vmem_limit_bytes=20 * 2**20),
        cost_estimate=pl.CostEstimate(
            flops=len(pairs) * 10**9, bytes_accessed=10**6, transcendentals=0
        ),
        name="visit",
    )(*args)


def field_kernel(coords, alpha, solves, probes, length, field, dist_ref, coup_ref):
    size = length.shape[1]
    spread = jnp.broadcast_to(length[...], (size, size))
    row = lax.broadcasted_iota(jnp.int32, (size, size), 0)
    col = lax.broadcasted_iota(jnp.int32, (size, size), 1)
    column = jnp.sum(jnp.where(row == col, spread, 0.0), 1, keepdims=True)
    scaled = coords[...] * (root_five / column)
    high, low = halves(scaled)
    near = high.astype(f32) + low.astype(f32)
    middle = DIM + GROUP
    field[0:DIM, :] = scaled
    field[DIM : DIM + 1, :] = alpha[...]
    field[DIM + 1 : middle, :] = solves[...]
    field[middle : middle + 1, :] = jnp.sum(near * near, 0, keepdims=True)
    field[middle + 1 :, :] = probes[...]
    own_forms(field[...], dist_ref, coup_ref)


def make_field(coords, alpha, solves, probes, lengthscale):
    points = coords.shape[1]
    return pl.pallas_call(
        field_kernel,
        out_shape=[
            jax.ShapeDtypeStruct((DIM + 2 * GROUP, points), f32),
            jax.ShapeDtypeStruct((4 * DIM + GROUP, points), bf16),
            jax.ShapeDtypeStruct((8 * GROUP, points), bf16),
        ],
        in_specs=[VMEM] * 5,
        out_specs=[VMEM] * 3,
        compiler_params=pltpu.CompilerParams(vmem_limit_bytes=8 * 2**20),
        name="field",
    )(coords, alpha[None], solves, probes, lengthscale[None])


def swapped(value):
    count = lax.axis_size("blk")
    return lax.ppermute(value, "blk", [(b, b + 1 - 2 * (b % 2)) for b in range(count)])


def toward(value, even, odd):
    count = lax.axis_size("blk")
    pairs = [(b, (b + (odd if b % 2 else even)) % count) for b in range(count)]
    return lax.ppermute(value, "blk", pairs)


def on_device(coords, alpha, probe_solves, probes, lengthscale):
    half_inv = 1.0 / (2.0 * probes.shape[0])
    hops = lax.axis_size("blk") // 8
    field, *own = make_field(coords, alpha, probe_solves, probes, lengthscale)
    near = toward(field, -2, 2)
    mate = swapped(field)
    cross = toward(field, 3, -3)
    acc, *own_mate = visit(half_inv, ((0, 0),), [mate], [own], [], n_form=1)
    accs = [acc]
    for hop in range(1, hops):
        here, there = near, cross
        near, cross = toward(here, -2, 2), toward(there, -2, 2)
        accs = visit(half_inv, ((0, 0), (0, 1)), [here], [own, own_mate], accs)
        accs = visit(half_inv, ((0, 0), (0, 1)), [there], [own, own_mate], accs)
    _, mine = visit(
        half_inv, ((0, 0),), [near], [own], accs[:1], done=(0,), fields=[field]
    )
    _, theirs = visit(
        half_inv, ((0, 0), (1, 0)), [near, cross], [own_mate], accs[1:], done=(0,), fields=[mate]
    )
    total = mine + swapped(theirs)
    return (-(root_five / 3.0) / lengthscale)[:, None] * total


def solution(mesh):
    return jax.shard_map(
        on_device,
        mesh=mesh,
        in_specs=(
            P(None, ("groups", "blk")),
            P(("groups", "blk")),
            P(None, ("groups", "blk")),
            P(None, ("groups", "blk")),
            P(),
        ),
        out_specs=P(None, ("groups", "blk")),
        check_vma=False,
    )
```

```python
import functools

import jax
import jax.numpy as jnp
from jax import lax
from jax.experimental import pallas as pl
from jax.experimental.pallas import tpu as pltpu
from jax.sharding import PartitionSpec as P

root_five = 5.0**0.5
minus_log2e = -1.4426950408889634
f32, bf16 = jnp.float32, jnp.bfloat16
VMEM = pl.BlockSpec(memory_space=pltpu.VMEM)
DIM, GROUP, SUMS = 32, 16, 80
STEP, BACK, AHEAD, LAG = 128, 256, 1, 2


def halves(value):
    high = value.astype(bf16)
    return high, (value - high.astype(f32)).astype(bf16)


def row_is(row, value, other):
    return jnp.where(lax.broadcasted_iota(jnp.int32, other.shape, 0) == row, value, other)


def edge_rows(square, parts_at, ones_at):
    one = square.astype(bf16).astype(f32)
    rest = square - one
    two = rest.astype(bf16).astype(f32)
    row = lax.broadcasted_iota(jnp.int32, square.shape, 0)
    edge = jnp.where((row >= ones_at) & (row < ones_at + 3), 1.0, 0.0)
    for index, part in enumerate((one, two, rest - two)):
        edge = row_is(parts_at + index, part, edge)
    return edge.astype(bf16)


def own_forms(field, dist_ref, coup_ref):
    high, low = halves(field[:DIM])
    first, second = field[DIM : DIM + GROUP], field[DIM + GROUP :]
    square = jnp.broadcast_to(second[:1], first.shape)
    dist_ref[...] = jnp.concatenate([high, low, high, low, edge_rows(square, 3, 0)], 0)
    table = jnp.concatenate([row_is(0, first, second), row_is(0, 0.0, first)], 0)
    high, low = halves(table)
    coup_ref[...] = jnp.concatenate([high, low, high, low], 0)


def visit_forms(half_inv, field, dist_ref, coup_ref, sums_ref):
    points = field.shape[1]
    high, low = halves(field[:DIM])
    first, second = field[DIM : DIM + GROUP], field[DIM + GROUP :]
    sums_ref[...] = jnp.concatenate([high, low, jnp.ones((GROUP, points), bf16)], 0)
    square = jnp.broadcast_to(second[:1], first.shape)
    twice = [-2.0 * high, -2.0 * low]
    zero = jnp.zeros((256 - 4 * DIM - GROUP, points), bf16)
    dist = jnp.concatenate([*twice, *twice[::-1], edge_rows(square, 0, 3), zero], 0)
    dist_ref[...] = dist.T
    table = jnp.concatenate(
        [row_is(0, first, -half_inv * first), row_is(0, 0.0, -half_inv * second)], 0
    )
    high, low = halves(table)
    coup_ref[...] = jnp.concatenate([high, high, low, low], 0).T


def weights(dist, coup):
    dist = jnp.maximum(dist, 1e-30)
    scaled = dist * lax.rsqrt(dist)
    return coup * ((1.0 + scaled) * jnp.exp2(scaled * minus_log2e))


def dot(left, right):
    return lax.dot_general(
        left, right, (((1,), (0,)), ((), ())), preferred_element_type=f32
    )


def add_tiles(pairs, sides, own, accs, high_ref, low_ref):
    points = accs[0].shape[1]
    width = high_ref.shape[2]
    depth = own[0][0].shape[0]
    chunks = [
        (v, o, start, begin)
        for v, o in pairs
        for start in range(0, points, width)
        for begin in range(0, points, STEP)
    ]

    def front(chunk):
        v, o, start, begin = chunk
        rows, cols = slice(begin, begin + STEP), slice(start, start + width)
        return (
            dot(sides[v][0][rows, :depth], own[o][0][:, cols]),
            dot(sides[v][1][rows, :], own[o][1][:, cols]),
        )

    def middle(chunk, products, slot):
        v, o, start, begin = chunk
        rows = slice(begin, begin + STEP)
        high, low = halves(weights(*products))
        high_ref[slot, rows, :] = high
        low_ref[slot, rows, :] = low

    def back(chunk, slot):
        v, o, start, begin = chunk
        sums = sides[v][2][:, begin : begin + BACK]
        rows, cols = slice(begin, begin + BACK), slice(start, start + width)
        accs[o][:, cols] += dot(sums, high_ref[slot, rows, :]) + dot(sums, low_ref[slot, rows, :])

    per = points // STEP
    slot_of = lambda index: (index // per) % 2
    per_back = BACK // STEP
    products = {}
    for index in range(min(AHEAD, len(chunks))):
        products[index] = front(chunks[index])
    for index, chunk in enumerate(chunks):
        if index + AHEAD < len(chunks):
            products[index + AHEAD] = front(chunks[index + AHEAD])
        middle(chunk, products.pop(index), slot_of(index))
        late = index - LAG
        if late >= 0 and late % per_back == per_back - 1:
            first = late - per_back + 1
            back(chunks[first], slot_of(first))
    for late in range(len(chunks) - LAG, len(chunks)):
        if late % per_back == per_back - 1:
            first = late - per_back + 1
            back(chunks[first], slot_of(first))


def finish(field, acc):
    high, low = halves(field[:DIM])
    near = high.astype(f32) + low.astype(f32)
    return near * acc[2 * DIM : 2 * DIM + 1] - (acc[:DIM] + acc[DIM : 2 * DIM])


def visit_kernel(half_inv, pairs, n_vis, n_own, n_acc, n_form, done, *refs):
    refs = list(refs)

    def take(count):
        taken, refs[:] = refs[:count], refs[count:]
        return taken

    vis = take(n_vis)
    own = [take(2) for _ in range(n_own)]
    acc_in = take(n_acc)
    fields = take(len(done))
    acc_out = take(n_own)
    forms = [take(2) for _ in range(n_form)]
    outs = take(len(done))
    high_ref, low_ref = take(2)
    for index in range(n_own):
        if index < n_acc:
            acc_out[index][...] = acc_in[index][...]
        else:
            acc_out[index][...] = jnp.zeros_like(acc_out[index])
    for index in range(n_form):
        own_forms(vis[index][...], *forms[index])
    sides = []
    for ref in vis:
        side = take(3)
        visit_forms(half_inv, ref[...], *side)
        sides.append(side)
    add_tiles(pairs, sides, own, acc_out, high_ref, low_ref)
    for o, field, out in zip(done, fields, outs):
        out[...] = finish(field[...], acc_out[o][...])


def visit(half_inv, pairs, vis, own, accs, n_form=0, done=(), fields=()):
    points = vis[0].shape[1]
    n_own = len(own)
    acc_shape = jax.ShapeDtypeStruct((SUMS, points), f32)
    form_shapes = [
        jax.ShapeDtypeStruct((4 * DIM + GROUP, points), bf16),
        jax.ShapeDtypeStruct((8 * GROUP, points), bf16),
    ]
    out_shape = [acc_shape] * n_own + form_shapes * n_form
    out_shape += [jax.ShapeDtypeStruct((DIM, points), f32)] * len(done)
    scratch = [pltpu.VMEM((2, points, 256), bf16)] * 2
    for _ in vis:
        scratch += [
            pltpu.VMEM((points, 256), bf16),
            pltpu.VMEM((points, 8 * GROUP), bf16),
            pltpu.VMEM((SUMS, points), bf16),
        ]
    args = [*vis, *[ref for forms in own for ref in forms], *accs, *fields]
    first = len(vis) + 2 * n_own
    return pl.pallas_call(
        functools.partial(
            visit_kernel, half_inv, pairs, len(vis), n_own, len(accs), n_form, done
        ),
        out_shape=out_shape,
        in_specs=[VMEM] * len(args),
        out_specs=[VMEM] * len(out_shape),
        scratch_shapes=scratch,
        input_output_aliases={first + index: index for index in range(len(accs))},
        compiler_params=pltpu.CompilerParams(vmem_limit_bytes=20 * 2**20, flags={}),
        cost_estimate=pl.CostEstimate(
            flops=len(pairs) * 10**9, bytes_accessed=10**6, transcendentals=0
        ),
        name="visit",
    )(*args)


def field_kernel(coords, alpha, solves, probes, length, field, dist_ref, coup_ref):
    size = length.shape[1]
    spread = jnp.broadcast_to(length[...], (size, size))
    row = lax.broadcasted_iota(jnp.int32, (size, size), 0)
    col = lax.broadcasted_iota(jnp.int32, (size, size), 1)
    column = jnp.sum(jnp.where(row == col, spread, 0.0), 1, keepdims=True)
    scaled = coords[...] * (1.0 / column)
    high, low = halves(scaled)
    near = high.astype(f32) + low.astype(f32)
    middle = DIM + GROUP
    lanes = alpha.shape[1]
    field[0:DIM, :] = scaled
    for index in range(alpha.shape[0]):
        field[DIM : DIM + 1, index * lanes : (index + 1) * lanes] = alpha[index : index + 1, :]
    field[DIM + 1 : middle, :] = solves[...]
    field[middle : middle + 1, :] = jnp.sum(near * near, 0, keepdims=True)
    field[middle + 1 :, :] = probes[...]
    own_forms(field[...], dist_ref, coup_ref)


def make_field(coords, alpha, solves, probes, lengthscale):
    points = coords.shape[1]
    args = (coords * root_five, alpha.reshape(-1, 128), solves, probes, lengthscale[None])
    return pl.pallas_call(
        field_kernel,
        out_shape=[
            jax.ShapeDtypeStruct((DIM + 2 * GROUP, points), f32),
            jax.ShapeDtypeStruct((4 * DIM + GROUP, points), bf16),
            jax.ShapeDtypeStruct((8 * GROUP, points), bf16),
        ],
        in_specs=[VMEM] * 5,
        out_specs=[VMEM] * 3,
        compiler_params=pltpu.CompilerParams(vmem_limit_bytes=8 * 2**20),
        name="field",
    )(*args)


def swapped(value):
    count = lax.axis_size("blk")
    return lax.ppermute(value, "blk", [(b, b + 1 - 2 * (b % 2)) for b in range(count)])


def toward(value, even, odd):
    count = lax.axis_size("blk")
    pairs = [(b, (b + (odd if b % 2 else even)) % count) for b in range(count)]
    return lax.ppermute(value, "blk", pairs)


def on_device(coords, alpha, probe_solves, probes, lengthscale):
    half_inv = 1.0 / (2.0 * probes.shape[0])
    hops = lax.axis_size("blk") // 8
    field, *own = make_field(coords, alpha, probe_solves, probes, lengthscale)
    mate = swapped(field)
    near = toward(field, -2, 2)
    cross = toward(field, 3, -3)
    acc, *own_mate = visit(half_inv, ((0, 0),), [mate], [own], [], n_form=1)
    near, cross, acc = lax.optimization_barrier((near, cross, acc))
    accs = [acc]
    for hop in range(1, hops):
        here, there = near, cross
        near = toward(here, -2, 2)
        accs = visit(half_inv, ((0, 1), (0, 0)), [here], [own, own_mate], accs)
        there, near_accs = lax.optimization_barrier((there, accs))
        cross = toward(there, -2, 2)
        accs = visit(half_inv, ((0, 1), (0, 0)), [there], [own, own_mate], near_accs)
    (acc,) = visit(half_inv, ((0, 0),), [near], [own_mate], accs[1:])
    cross, acc = lax.optimization_barrier((cross, acc))
    _, theirs = visit(half_inv, ((0, 0),), [cross], [own_mate], [acc], done=(0,), fields=[mate])
    theirs = swapped(theirs)
    _, mine = visit(half_inv, ((0, 0),), [near], [own], accs[:1], done=(0,), fields=[field])
    total = mine + theirs
    return (-(root_five / 3.0) / lengthscale)[:, None] * total


def solution(mesh):
    return jax.shard_map(
        on_device,
        mesh=mesh,
        in_specs=(
            P(None, ("groups", "blk")),
            P(("groups", "blk")),
            P(None, ("groups", "blk")),
            P(None, ("groups", "blk")),
            P(),
        ),
        out_specs=P(None, ("groups", "blk")),
        check_vma=False,
    )
```

```python
import functools

import jax
import jax.numpy as jnp
from jax import lax
from jax.experimental import pallas as pl
from jax.experimental.pallas import tpu as pltpu
from jax.sharding import PartitionSpec as P

root_five = 5.0**0.5
minus_log2e = -1.4426950408889634
f32, bf16 = jnp.float32, jnp.bfloat16
VMEM = pl.BlockSpec(memory_space=pltpu.VMEM)
DIM, GROUP, SUMS = 32, 16, 80
STEP, BACK, AHEAD, LAG = 128, 256, 1, 2


def halves(value):
    high = value.astype(bf16)
    return high, (value - high.astype(f32)).astype(bf16)


def row_is(row, value, other):
    return jnp.where(lax.broadcasted_iota(jnp.int32, other.shape, 0) == row, value, other)


def edge_rows(square, parts_at, ones_at):
    one = square.astype(bf16).astype(f32)
    rest = square - one
    two = rest.astype(bf16).astype(f32)
    row = lax.broadcasted_iota(jnp.int32, square.shape, 0)
    edge = jnp.where((row >= ones_at) & (row < ones_at + 3), 1.0, 0.0)
    for index, part in enumerate((one, two, rest - two)):
        edge = row_is(parts_at + index, part, edge)
    return edge.astype(bf16)


def own_forms(field, dist_ref, coup_ref):
    high, low = halves(field[:DIM])
    first, second = field[DIM : DIM + GROUP], field[DIM + GROUP :]
    square = jnp.broadcast_to(second[:1], first.shape)
    dist_ref[...] = jnp.concatenate([high, low, high, low, edge_rows(square, 3, 0)], 0)
    table = jnp.concatenate([row_is(0, first, second), row_is(0, 0.0, first)], 0)
    high, low = halves(table)
    coup_ref[...] = jnp.concatenate([high, low, high, low], 0)


def visit_forms(half_inv, field, dist_ref, coup_ref, sums_ref):
    points = field.shape[1]
    high, low = halves(field[:DIM])
    first, second = field[DIM : DIM + GROUP], field[DIM + GROUP :]
    sums_ref[...] = jnp.concatenate([high, low, jnp.ones((GROUP, points), bf16)], 0)
    square = jnp.broadcast_to(second[:1], first.shape)
    twice = [-2.0 * high, -2.0 * low]
    zero = jnp.zeros((256 - 4 * DIM - GROUP, points), bf16)
    dist = jnp.concatenate([*twice, *twice[::-1], edge_rows(square, 0, 3), zero], 0)
    dist_ref[...] = dist.T
    table = jnp.concatenate(
        [row_is(0, first, -half_inv * first), row_is(0, 0.0, -half_inv * second)], 0
    )
    high, low = halves(table)
    coup_ref[...] = jnp.concatenate([high, high, low, low], 0).T


def weights(dist, coup):
    dist = jnp.maximum(dist, 1e-30)
    scaled = dist * lax.rsqrt(dist)
    return coup * ((1.0 + scaled) * jnp.exp2(scaled * minus_log2e))


def dot(left, right):
    return lax.dot_general(
        left, right, (((1,), (0,)), ((), ())), preferred_element_type=f32
    )


def add_tiles(pairs, sides, own, accs, high_ref, low_ref):
    points = accs[0].shape[1]
    width = high_ref.shape[2]
    depth = own[0][0].shape[0]
    chunks = [
        (v, o, start, begin)
        for v, o in pairs
        for start in range(0, points, width)
        for begin in range(0, points, STEP)
    ]

    def front(chunk):
        v, o, start, begin = chunk
        rows, cols = slice(begin, begin + STEP), slice(start, start + width)
        return (
            dot(sides[v][0][rows, :depth], own[o][0][:, cols]),
            dot(sides[v][1][rows, :], own[o][1][:, cols]),
        )

    def middle(chunk, products, slot):
        v, o, start, begin = chunk
        rows = slice(begin, begin + STEP)
        high, low = halves(weights(*products))
        high_ref[slot, rows, :] = high
        low_ref[slot, rows, :] = low

    def back(chunk, slot):
        v, o, start, begin = chunk
        sums = sides[v][2][:, begin : begin + BACK]
        rows, cols = slice(begin, begin + BACK), slice(start, start + width)
        accs[o][:, cols] += dot(sums, high_ref[slot, rows, :]) + dot(sums, low_ref[slot, rows, :])

    per = points // STEP
    slot_of = lambda index: (index // per) % 2
    per_back = BACK // STEP
    products = {}
    for index in range(min(AHEAD, len(chunks))):
        products[index] = front(chunks[index])
    for index, chunk in enumerate(chunks):
        if index + AHEAD < len(chunks):
            products[index + AHEAD] = front(chunks[index + AHEAD])
        middle(chunk, products.pop(index), slot_of(index))
        late = index - LAG
        if late >= 0 and late % per_back == per_back - 1:
            first = late - per_back + 1
            back(chunks[first], slot_of(first))
    for late in range(len(chunks) - LAG, len(chunks)):
        if late % per_back == per_back - 1:
            first = late - per_back + 1
            back(chunks[first], slot_of(first))


def finish(field, acc):
    high, low = halves(field[:DIM])
    near = high.astype(f32) + low.astype(f32)
    return near * acc[2 * DIM : 2 * DIM + 1] - (acc[:DIM] + acc[DIM : 2 * DIM])


def visit_kernel(half_inv, pairs, n_vis, n_own, n_acc, n_form, done, *refs):
    refs = list(refs)

    def take(count):
        taken, refs[:] = refs[:count], refs[count:]
        return taken

    vis = take(n_vis)
    own = [take(2) for _ in range(n_own)]
    acc_in = take(n_acc)
    fields = take(len(done))
    acc_out = take(n_own)
    forms = [take(2) for _ in range(n_form)]
    outs = take(len(done))
    high_ref, low_ref = take(2)
    for index in range(n_own):
        if index < n_acc:
            acc_out[index][...] = acc_in[index][...]
        else:
            acc_out[index][...] = jnp.zeros_like(acc_out[index])
    for index in range(n_form):
        own_forms(vis[index][...], *forms[index])
    sides = []
    for ref in vis:
        side = take(3)
        visit_forms(half_inv, ref[...], *side)
        sides.append(side)
    add_tiles(pairs, sides, own, acc_out, high_ref, low_ref)
    for o, field, out in zip(done, fields, outs):
        out[...] = finish(field[...], acc_out[o][...])


def visit(half_inv, pairs, vis, own, accs, n_form=0, done=(), fields=()):
    points = vis[0].shape[1]
    n_own = len(own)
    acc_shape = jax.ShapeDtypeStruct((SUMS, points), f32)
    form_shapes = [
        jax.ShapeDtypeStruct((4 * DIM + GROUP, points), bf16),
        jax.ShapeDtypeStruct((8 * GROUP, points), bf16),
    ]
    out_shape = [acc_shape] * n_own + form_shapes * n_form
    out_shape += [jax.ShapeDtypeStruct((DIM, points), f32)] * len(done)
    scratch = [pltpu.VMEM((2, points, 256), bf16)] * 2
    for _ in vis:
        scratch += [
            pltpu.VMEM((points, 256), bf16),
            pltpu.VMEM((points, 8 * GROUP), bf16),
            pltpu.VMEM((SUMS, points), bf16),
        ]
    args = [*vis, *[ref for forms in own for ref in forms], *accs, *fields]
    first = len(vis) + 2 * n_own
    return pl.pallas_call(
        functools.partial(
            visit_kernel, half_inv, pairs, len(vis), n_own, len(accs), n_form, done
        ),
        out_shape=out_shape,
        in_specs=[VMEM] * len(args),
        out_specs=[VMEM] * len(out_shape),
        scratch_shapes=scratch,
        input_output_aliases={first + index: index for index in range(len(accs))},
        compiler_params=pltpu.CompilerParams(vmem_limit_bytes=20 * 2**20),
        cost_estimate=pl.CostEstimate(
            flops=len(pairs) * 10**9, bytes_accessed=10**6, transcendentals=0
        ),
        name="visit",
    )(*args)


def field_kernel(coords, alpha, solves, probes, length, field, dist_ref, coup_ref):
    size = length.shape[1]
    spread = jnp.broadcast_to(length[...], (size, size))
    row = lax.broadcasted_iota(jnp.int32, (size, size), 0)
    col = lax.broadcasted_iota(jnp.int32, (size, size), 1)
    column = jnp.sum(jnp.where(row == col, spread, 0.0), 1, keepdims=True)
    scaled = coords[...] * (1.0 / column)
    high, low = halves(scaled)
    near = high.astype(f32) + low.astype(f32)
    middle = DIM + GROUP
    lanes = alpha.shape[1]
    field[0:DIM, :] = scaled
    for index in range(alpha.shape[0]):
        field[DIM : DIM + 1, index * lanes : (index + 1) * lanes] = alpha[index : index + 1, :]
    field[DIM + 1 : middle, :] = solves[...]
    field[middle : middle + 1, :] = jnp.sum(near * near, 0, keepdims=True)
    field[middle + 1 :, :] = probes[...]
    own_forms(field[...], dist_ref, coup_ref)


def make_field(coords, alpha, solves, probes, lengthscale):
    points = coords.shape[1]
    args = (coords * root_five, alpha.reshape(-1, 128), solves, probes, lengthscale[None])
    return pl.pallas_call(
        field_kernel,
        out_shape=[
            jax.ShapeDtypeStruct((DIM + 2 * GROUP, points), f32),
            jax.ShapeDtypeStruct((4 * DIM + GROUP, points), bf16),
            jax.ShapeDtypeStruct((8 * GROUP, points), bf16),
        ],
        in_specs=[VMEM] * 5,
        out_specs=[VMEM] * 3,
        compiler_params=pltpu.CompilerParams(vmem_limit_bytes=8 * 2**20),
        name="field",
    )(*args)


def swapped(value):
    count = lax.axis_size("blk")
    return lax.ppermute(value, "blk", [(b, b + 1 - 2 * (b % 2)) for b in range(count)])


def toward(value, even, odd):
    count = lax.axis_size("blk")
    pairs = [(b, (b + (odd if b % 2 else even)) % count) for b in range(count)]
    return lax.ppermute(value, "blk", pairs)


def on_device(coords, alpha, probe_solves, probes, lengthscale):
    half_inv = 1.0 / (2.0 * probes.shape[0])
    hops = lax.axis_size("blk") // 8
    field, *own = make_field(coords, alpha, probe_solves, probes, lengthscale)
    mate = swapped(field)
    near = toward(field, -2, 2)
    acc, *own_mate = visit(half_inv, ((0, 0),), [mate], [own], [], n_form=1)
    later, acc = lax.optimization_barrier((field, acc))
    cross = toward(later, 3, -3)
    near, acc = lax.optimization_barrier((near, acc))
    accs = [acc]
    for hop in range(1, hops):
        here, there = near, cross
        near = toward(here, -2, 2)
        accs = visit(half_inv, ((0, 1), (0, 0)), [here], [own, own_mate], accs)
        there, near_accs = lax.optimization_barrier((there, accs))
        cross = toward(there, -2, 2)
        accs = visit(half_inv, ((0, 1), (0, 0)), [there], [own, own_mate], near_accs)
    (acc,) = visit(half_inv, ((0, 0),), [near], [own_mate], accs[1:])
    cross, acc = lax.optimization_barrier((cross, acc))
    _, theirs = visit(half_inv, ((0, 0),), [cross], [own_mate], [acc], done=(0,), fields=[mate])
    theirs = swapped(theirs)
    _, mine = visit(half_inv, ((0, 0),), [near], [own], accs[:1], done=(0,), fields=[field])
    total = mine + theirs
    return (-(root_five / 3.0) / lengthscale)[:, None] * total


def solution(mesh):
    return jax.shard_map(
        on_device,
        mesh=mesh,
        in_specs=(
            P(None, ("groups", "blk")),
            P(("groups", "blk")),
            P(None, ("groups", "blk")),
            P(None, ("groups", "blk")),
            P(),
        ),
        out_specs=P(None, ("groups", "blk")),
        check_vma=False,
    )
```

```python
import functools

import jax
import jax.numpy as jnp
from jax import lax
from jax.experimental import pallas as pl
from jax.experimental.pallas import tpu as pltpu
from jax.sharding import PartitionSpec as P

root_five = 5.0**0.5
minus_log2e = -1.4426950408889634
f32, bf16 = jnp.float32, jnp.bfloat16
VMEM = pl.BlockSpec(memory_space=pltpu.VMEM)
DIM, GROUP, SUMS = 32, 16, 80
STEP, BACK, AHEAD, LAG = 192, 192, 1, 1


def halves(value):
    high = value.astype(bf16)
    return high, (value - high.astype(f32)).astype(bf16)


def row_is(row, value, other):
    return jnp.where(lax.broadcasted_iota(jnp.int32, other.shape, 0) == row, value, other)


def edge_rows(square, parts_at, ones_at):
    one = square.astype(bf16).astype(f32)
    rest = square - one
    two = rest.astype(bf16).astype(f32)
    row = lax.broadcasted_iota(jnp.int32, square.shape, 0)
    edge = jnp.where((row >= ones_at) & (row < ones_at + 3), 1.0, 0.0)
    for index, part in enumerate((one, two, rest - two)):
        edge = row_is(parts_at + index, part, edge)
    return edge.astype(bf16)


def own_forms(field, dist_ref, coup_ref):
    high, low = halves(field[:DIM])
    first, second = field[DIM : DIM + GROUP], field[DIM + GROUP :]
    square = jnp.broadcast_to(second[:1], first.shape)
    dist_ref[...] = jnp.concatenate([high, low, high, low, edge_rows(square, 3, 0)], 0)
    table = jnp.concatenate([row_is(0, first, second), row_is(0, 0.0, first)], 0)
    high, low = halves(table)
    coup_ref[...] = jnp.concatenate([high, low, high, low], 0)


def visit_forms(half_inv, field, dist_ref, coup_ref, sums_ref):
    points = field.shape[1]
    high, low = halves(field[:DIM])
    first, second = field[DIM : DIM + GROUP], field[DIM + GROUP :]
    sums_ref[...] = jnp.concatenate([high, low, jnp.ones((GROUP, points), bf16)], 0)
    square = jnp.broadcast_to(second[:1], first.shape)
    twice = [-2.0 * high, -2.0 * low]
    zero = jnp.zeros((256 - 4 * DIM - GROUP, points), bf16)
    dist = jnp.concatenate([*twice, *twice[::-1], edge_rows(square, 0, 3), zero], 0)
    dist_ref[...] = dist.T
    table = jnp.concatenate(
        [row_is(0, first, -half_inv * first), row_is(0, 0.0, -half_inv * second)], 0
    )
    high, low = halves(table)
    coup_ref[...] = jnp.concatenate([high, high, low, low], 0).T


def weights(dist, coup):
    dist = jnp.maximum(dist, 1e-30)
    scaled = dist * lax.rsqrt(dist)
    return coup * ((1.0 + scaled) * jnp.exp2(scaled * minus_log2e))


def dot(left, right):
    return lax.dot_general(
        left, right, (((1,), (0,)), ((), ())), preferred_element_type=f32
    )


def add_tiles(pairs, sides, own, accs, high_ref, low_ref):
    points = accs[0].shape[1]
    width = high_ref.shape[2]
    depth = own[0][0].shape[0]
    chunks = [
        (v, o, start, begin)
        for v, o in pairs
        for start in range(0, points, width)
        for begin in range(0, points, STEP)
    ]

    def front(chunk):
        v, o, start, begin = chunk
        rows, cols = slice(begin, begin + STEP), slice(start, start + width)
        return (
            dot(sides[v][0][rows, :depth], own[o][0][:, cols]),
            dot(sides[v][1][rows, :], own[o][1][:, cols]),
        )

    def middle(chunk, products, slot):
        v, o, start, begin = chunk
        rows = slice(begin, begin + STEP)
        high, low = halves(weights(*products))
        high_ref[slot, rows, :] = high
        low_ref[slot, rows, :] = low

    def back(chunk, slot):
        v, o, start, begin = chunk
        sums = sides[v][2][:, begin : begin + BACK]
        rows, cols = slice(begin, begin + BACK), slice(start, start + width)
        accs[o][:, cols] += dot(sums, high_ref[slot, rows, :]) + dot(sums, low_ref[slot, rows, :])

    per = points // STEP
    slot_of = lambda index: (index // per) % 2
    per_back = BACK // STEP
    products = {}
    for index in range(min(AHEAD, len(chunks))):
        products[index] = front(chunks[index])
    for index, chunk in enumerate(chunks):
        if index + AHEAD < len(chunks):
            products[index + AHEAD] = front(chunks[index + AHEAD])
        middle(chunk, products.pop(index), slot_of(index))
        late = index - LAG
        if late >= 0 and late % per_back == per_back - 1:
            first = late - per_back + 1
            back(chunks[first], slot_of(first))
    for late in range(len(chunks) - LAG, len(chunks)):
        if late % per_back == per_back - 1:
            first = late - per_back + 1
            back(chunks[first], slot_of(first))


def finish(field, acc):
    high, low = halves(field[:DIM])
    near = high.astype(f32) + low.astype(f32)
    return near * acc[2 * DIM : 2 * DIM + 1] - (acc[:DIM] + acc[DIM : 2 * DIM])


def visit_kernel(half_inv, pairs, n_vis, n_own, n_acc, n_form, done, *refs):
    refs = list(refs)

    def take(count):
        taken, refs[:] = refs[:count], refs[count:]
        return taken

    vis = take(n_vis)
    own = [take(2) for _ in range(n_own)]
    acc_in = take(n_acc)
    fields = take(len(done))
    acc_out = take(n_own)
    forms = [take(2) for _ in range(n_form)]
    outs = take(len(done))
    high_ref, low_ref = take(2)
    for index in range(n_own):
        if index < n_acc:
            acc_out[index][...] = acc_in[index][...]
        else:
            acc_out[index][...] = jnp.zeros_like(acc_out[index])
    for index in range(n_form):
        own_forms(vis[index][...], *forms[index])
    sides = []
    for ref in vis:
        side = take(3)
        visit_forms(half_inv, ref[...], *side)
        sides.append(side)
    add_tiles(pairs, sides, own, acc_out, high_ref, low_ref)
    for o, field, out in zip(done, fields, outs):
        out[...] = finish(field[...], acc_out[o][...])


def visit(half_inv, pairs, vis, own, accs, n_form=0, done=(), fields=()):
    points = vis[0].shape[1]
    n_own = len(own)
    acc_shape = jax.ShapeDtypeStruct((SUMS, points), f32)
    form_shapes = [
        jax.ShapeDtypeStruct((4 * DIM + GROUP, points), bf16),
        jax.ShapeDtypeStruct((8 * GROUP, points), bf16),
    ]
    out_shape = [acc_shape] * n_own + form_shapes * n_form
    out_shape += [jax.ShapeDtypeStruct((DIM, points), f32)] * len(done)
    scratch = [pltpu.VMEM((2, points, 256), bf16)] * 2
    for _ in vis:
        scratch += [
            pltpu.VMEM((points, 256), bf16),
            pltpu.VMEM((points, 8 * GROUP), bf16),
            pltpu.VMEM((SUMS, points), bf16),
        ]
    args = [*vis, *[ref for forms in own for ref in forms], *accs, *fields]
    first = len(vis) + 2 * n_own
    return pl.pallas_call(
        functools.partial(
            visit_kernel, half_inv, pairs, len(vis), n_own, len(accs), n_form, done
        ),
        out_shape=out_shape,
        in_specs=[VMEM] * len(args),
        out_specs=[VMEM] * len(out_shape),
        scratch_shapes=scratch,
        input_output_aliases={first + index: index for index in range(len(accs))},
        compiler_params=pltpu.CompilerParams(vmem_limit_bytes=20 * 2**20),
        cost_estimate=pl.CostEstimate(
            flops=len(pairs) * 10**9, bytes_accessed=10**6, transcendentals=0
        ),
        name="visit",
    )(*args)


def field_kernel(coords, alpha, solves, probes, length, field, dist_ref, coup_ref):
    size = length.shape[1]
    spread = jnp.broadcast_to(length[...], (size, size))
    row = lax.broadcasted_iota(jnp.int32, (size, size), 0)
    col = lax.broadcasted_iota(jnp.int32, (size, size), 1)
    column = jnp.sum(jnp.where(row == col, spread, 0.0), 1, keepdims=True)
    scaled = coords[...] * (1.0 / column)
    high, low = halves(scaled)
    near = high.astype(f32) + low.astype(f32)
    middle = DIM + GROUP
    lanes = alpha.shape[1]
    field[0:DIM, :] = scaled
    for index in range(alpha.shape[0]):
        field[DIM : DIM + 1, index * lanes : (index + 1) * lanes] = alpha[index : index + 1, :]
    field[DIM + 1 : middle, :] = solves[...]
    field[middle : middle + 1, :] = jnp.sum(near * near, 0, keepdims=True)
    field[middle + 1 :, :] = probes[...]
    own_forms(field[...], dist_ref, coup_ref)


def make_field(coords, alpha, solves, probes, lengthscale):
    points = coords.shape[1]
    args = (coords * root_five, alpha.reshape(-1, 128), solves, probes, lengthscale[None])
    return pl.pallas_call(
        field_kernel,
        out_shape=[
            jax.ShapeDtypeStruct((DIM + 2 * GROUP, points), f32),
            jax.ShapeDtypeStruct((4 * DIM + GROUP, points), bf16),
            jax.ShapeDtypeStruct((8 * GROUP, points), bf16),
        ],
        in_specs=[VMEM] * 5,
        out_specs=[VMEM] * 3,
        compiler_params=pltpu.CompilerParams(vmem_limit_bytes=8 * 2**20),
        name="field",
    )(*args)


def swapped(value):
    count = lax.axis_size("blk")
    return lax.ppermute(value, "blk", [(b, b + 1 - 2 * (b % 2)) for b in range(count)])


def toward(value, even, odd):
    count = lax.axis_size("blk")
    pairs = [(b, (b + (odd if b % 2 else even)) % count) for b in range(count)]
    return lax.ppermute(value, "blk", pairs)


def on_device(coords, alpha, probe_solves, probes, lengthscale):
    half_inv = 1.0 / (2.0 * probes.shape[0])
    hops = lax.axis_size("blk") // 8
    field, *own = make_field(coords, alpha, probe_solves, probes, lengthscale)
    mate = swapped(field)
    near = toward(field, -2, 2)
    acc, *own_mate = visit(half_inv, ((0, 0),), [mate], [own], [], n_form=1)
    later, acc = lax.optimization_barrier((field, acc))
    cross = toward(later, 3, -3)
    near, acc = lax.optimization_barrier((near, acc))
    accs = [acc]
    for hop in range(1, hops):
        here, there = near, cross
        near = toward(here, -2, 2)
        accs = visit(half_inv, ((0, 1), (0, 0)), [here], [own, own_mate], accs)
        there, near_accs = lax.optimization_barrier((there, accs))
        cross = toward(there, -2, 2)
        accs = visit(half_inv, ((0, 1), (0, 0)), [there], [own, own_mate], near_accs)
    (acc,) = visit(half_inv, ((0, 0),), [near], [own_mate], accs[1:])
    cross, acc = lax.optimization_barrier((cross, acc))
    _, theirs = visit(half_inv, ((0, 0),), [cross], [own_mate], [acc], done=(0,), fields=[mate])
    theirs = swapped(theirs)
    _, mine = visit(half_inv, ((0, 0),), [near], [own], accs[:1], done=(0,), fields=[field])
    total = mine + theirs
    return (-(root_five / 3.0) / lengthscale)[:, None] * total


def solution(mesh):
    return jax.shard_map(
        on_device,
        mesh=mesh,
        in_specs=(
            P(None, ("groups", "blk")),
            P(("groups", "blk")),
            P(None, ("groups", "blk")),
            P(None, ("groups", "blk")),
            P(),
        ),
        out_specs=P(None, ("groups", "blk")),
        check_vma=False,
    )
```

```python
import functools

import jax
import jax.numpy as jnp
from jax import lax
from jax.experimental import pallas as pl
from jax.experimental.pallas import tpu as pltpu
from jax.sharding import PartitionSpec as P

root_five = 5.0**0.5
minus_log2e = -1.4426950408889634
f32, bf16 = jnp.float32, jnp.bfloat16
VMEM = pl.BlockSpec(memory_space=pltpu.VMEM)
DIM, GROUP, SUMS = 32, 16, 80
STEP, BACK, AHEAD, LAG = 192, 192, 1, 1


def halves(value):
    high = value.astype(bf16)
    return high, (value - high.astype(f32)).astype(bf16)


def row_is(row, value, other):
    return jnp.where(lax.broadcasted_iota(jnp.int32, other.shape, 0) == row, value, other)


def edge_rows(square, parts_at, ones_at):
    one = square.astype(bf16).astype(f32)
    rest = square - one
    two = rest.astype(bf16).astype(f32)
    row = lax.broadcasted_iota(jnp.int32, square.shape, 0)
    edge = jnp.where((row >= ones_at) & (row < ones_at + 3), 1.0, 0.0)
    for index, part in enumerate((one, two, rest - two)):
        edge = row_is(parts_at + index, part, edge)
    return edge.astype(bf16)


def scaled_halves(field, scale):
    wide = jnp.concatenate([scale] * (field.shape[1] // scale.shape[1]), 1)
    high, low = halves(field[:DIM] * wide)
    return high, low, high.astype(f32) + low.astype(f32)


def own_forms(field, scale, dist_ref, coup_ref):
    high, low, near = scaled_halves(field, scale)
    first, second = field[DIM : DIM + GROUP], field[DIM + GROUP :]
    square = jnp.broadcast_to(jnp.sum(near * near, 0, keepdims=True), first.shape)
    dist_ref[...] = jnp.concatenate([high, low, high, low, edge_rows(square, 3, 0)], 0)
    table = jnp.concatenate([row_is(0, first, second), row_is(0, 0.0, first)], 0)
    high, low = halves(table)
    coup_ref[...] = jnp.concatenate([high, low, high, low], 0)


def visit_forms(half_inv, field, scale, dist_ref, coup_ref, sums_ref):
    points = field.shape[1]
    high, low, near = scaled_halves(field, scale)
    first, second = field[DIM : DIM + GROUP], field[DIM + GROUP :]
    sums_ref[...] = jnp.concatenate([high, low, jnp.ones((GROUP, points), bf16)], 0)
    square = jnp.broadcast_to(jnp.sum(near * near, 0, keepdims=True), first.shape)
    twice = [-2.0 * high, -2.0 * low]
    zero = jnp.zeros((256 - 4 * DIM - GROUP, points), bf16)
    dist = jnp.concatenate([*twice, *twice[::-1], edge_rows(square, 0, 3), zero], 0)
    dist_ref[...] = dist.T
    table = jnp.concatenate(
        [row_is(0, first, -half_inv * first), row_is(0, 0.0, -half_inv * second)], 0
    )
    high, low = halves(table)
    coup_ref[...] = jnp.concatenate([high, high, low, low], 0).T


def weights(dist, coup):
    dist = jnp.maximum(dist, 1e-30)
    scaled = dist * lax.rsqrt(dist)
    return coup * ((1.0 + scaled) * jnp.exp2(scaled * minus_log2e))


def dot(left, right):
    return lax.dot_general(
        left, right, (((1,), (0,)), ((), ())), preferred_element_type=f32
    )


def add_tiles(pairs, sides, own, accs, high_ref, low_ref):
    points = accs[0].shape[1]
    width = high_ref.shape[2]
    depth = own[0][0].shape[0]
    chunks = [
        (v, o, start, begin)
        for v, o in pairs
        for start in range(0, points, width)
        for begin in range(0, points, STEP)
    ]

    def front(chunk):
        v, o, start, begin = chunk
        rows, cols = slice(begin, begin + STEP), slice(start, start + width)
        return (
            dot(sides[v][0][rows, :depth], own[o][0][:, cols]),
            dot(sides[v][1][rows, :], own[o][1][:, cols]),
        )

    def middle(chunk, products, slot):
        v, o, start, begin = chunk
        rows = slice(begin, begin + STEP)
        high, low = halves(weights(*products))
        high_ref[slot, rows, :] = high
        low_ref[slot, rows, :] = low

    def back(chunk, slot):
        v, o, start, begin = chunk
        sums = sides[v][2][:, begin : begin + BACK]
        rows, cols = slice(begin, begin + BACK), slice(start, start + width)
        accs[o][:, cols] += dot(sums, high_ref[slot, rows, :]) + dot(sums, low_ref[slot, rows, :])

    per = points // STEP
    slot_of = lambda index: (index // per) % 2
    per_back = BACK // STEP
    products = {}
    for index in range(min(AHEAD, len(chunks))):
        products[index] = front(chunks[index])
    for index, chunk in enumerate(chunks):
        if index + AHEAD < len(chunks):
            products[index + AHEAD] = front(chunks[index + AHEAD])
        middle(chunk, products.pop(index), slot_of(index))
        late = index - LAG
        if late >= 0 and late % per_back == per_back - 1:
            first = late - per_back + 1
            back(chunks[first], slot_of(first))
    for late in range(len(chunks) - LAG, len(chunks)):
        if late % per_back == per_back - 1:
            first = late - per_back + 1
            back(chunks[first], slot_of(first))


def finish(field, scale, acc):
    near = scaled_halves(field, scale)[2]
    return near * acc[2 * DIM : 2 * DIM + 1] - (acc[:DIM] + acc[DIM : 2 * DIM])


def visit_kernel(half_inv, pairs, n_vis, n_own, n_acc, n_form, done, *refs):
    refs = list(refs)

    def take(count):
        taken, refs[:] = refs[:count], refs[count:]
        return taken

    (scale,) = take(1)
    vis = take(n_vis)
    own = [take(2) for _ in range(n_own)]
    acc_in = take(n_acc)
    fields = take(len(done))
    acc_out = take(n_own)
    forms = [take(2) for _ in range(n_form)]
    outs = take(len(done))
    high_ref, low_ref = take(2)
    for index in range(n_own):
        if index < n_acc:
            acc_out[index][...] = acc_in[index][...]
        else:
            acc_out[index][...] = jnp.zeros_like(acc_out[index])
    for index in range(n_form):
        own_forms(vis[index][...], scale[...], *forms[index])
    sides = []
    for ref in vis:
        side = take(3)
        visit_forms(half_inv, ref[...], scale[...], *side)
        sides.append(side)
    add_tiles(pairs, sides, own, acc_out, high_ref, low_ref)
    for o, field, out in zip(done, fields, outs):
        out[...] = finish(field[...], scale[...], acc_out[o][...])


def visit(half_inv, scale, pairs, vis, own, accs, n_form=0, done=(), fields=()):
    points = vis[0].shape[1]
    n_own = len(own)
    acc_shape = jax.ShapeDtypeStruct((SUMS, points), f32)
    form_shapes = [
        jax.ShapeDtypeStruct((4 * DIM + GROUP, points), bf16),
        jax.ShapeDtypeStruct((8 * GROUP, points), bf16),
    ]
    out_shape = [acc_shape] * n_own + form_shapes * n_form
    out_shape += [jax.ShapeDtypeStruct((DIM, points), f32)] * len(done)
    scratch = [pltpu.VMEM((2, points, 256), bf16)] * 2
    for _ in vis:
        scratch += [
            pltpu.VMEM((points, 256), bf16),
            pltpu.VMEM((points, 8 * GROUP), bf16),
            pltpu.VMEM((SUMS, points), bf16),
        ]
    args = [scale, *vis, *[ref for forms in own for ref in forms], *accs, *fields]
    first = 1 + len(vis) + 2 * n_own
    return pl.pallas_call(
        functools.partial(
            visit_kernel, half_inv, pairs, len(vis), n_own, len(accs), n_form, done
        ),
        out_shape=out_shape,
        in_specs=[VMEM] * len(args),
        out_specs=[VMEM] * len(out_shape),
        scratch_shapes=scratch,
        input_output_aliases={first + index: index for index in range(len(accs))},
        compiler_params=pltpu.CompilerParams(vmem_limit_bytes=20 * 2**20),
        cost_estimate=pl.CostEstimate(
            flops=len(pairs) * 10**9, bytes_accessed=10**6, transcendentals=0
        ),
        name="visit",
    )(*args)


def field_kernel(coords, alpha, solves, probes, field):
    middle = DIM + GROUP
    lanes = alpha.shape[1]
    field[0:DIM, :] = coords[...]
    for index in range(alpha.shape[0]):
        cols = slice(index * lanes, (index + 1) * lanes)
        field[DIM : DIM + 1, cols] = alpha[index : index + 1, :]
        field[middle : middle + 1, cols] = alpha[index : index + 1, :]
    field[DIM + 1 : middle, :] = solves[...]
    field[middle + 1 :, :] = probes[...]


def make_field(coords, alpha, solves, probes):
    args = (coords * root_five, alpha.reshape(-1, 128), solves, probes)
    return pl.pallas_call(
        field_kernel,
        out_shape=jax.ShapeDtypeStruct((DIM + 2 * GROUP, coords.shape[1]), f32),
        in_specs=[VMEM] * len(args),
        out_specs=VMEM,
        compiler_params=pltpu.CompilerParams(vmem_limit_bytes=8 * 2**20),
        name="field",
    )(*args)


def scale_kernel(field, length, scale_ref, dist_ref, coup_ref):
    size = length.shape[1]
    spread = jnp.broadcast_to(length[...], (size, size))
    row = lax.broadcasted_iota(jnp.int32, (size, size), 0)
    col = lax.broadcasted_iota(jnp.int32, (size, size), 1)
    column = jnp.sum(jnp.where(row == col, spread, 0.0), 1, keepdims=True)
    scale = jnp.broadcast_to(1.0 / column, scale_ref.shape)
    scale_ref[...] = scale
    own_forms(field[...], scale, dist_ref, coup_ref)


def make_own(field, lengthscale):
    points = field.shape[1]
    return pl.pallas_call(
        scale_kernel,
        out_shape=[
            jax.ShapeDtypeStruct((DIM, 128), f32),
            jax.ShapeDtypeStruct((4 * DIM + GROUP, points), bf16),
            jax.ShapeDtypeStruct((8 * GROUP, points), bf16),
        ],
        in_specs=[VMEM] * 2,
        out_specs=[VMEM] * 3,
        compiler_params=pltpu.CompilerParams(vmem_limit_bytes=8 * 2**20),
        name="own",
    )(field, lengthscale[None])


def swapped(value):
    count = lax.axis_size("blk")
    return lax.ppermute(value, "blk", [(b, b + 1 - 2 * (b % 2)) for b in range(count)])


def toward(value, even, odd):
    count = lax.axis_size("blk")
    pairs = [(b, (b + (odd if b % 2 else even)) % count) for b in range(count)]
    return lax.ppermute(value, "blk", pairs)


def on_device(coords, alpha, probe_solves, probes, lengthscale):
    half_inv = 1.0 / (2.0 * probes.shape[0])
    hops = lax.axis_size("blk") // 8
    field = make_field(coords, alpha, probe_solves, probes)
    mate = swapped(field)
    near = toward(field, -2, 2)
    scale, *own = make_own(field, lengthscale)
    mate, own = lax.optimization_barrier((mate, own))
    acc, *own_mate = visit(half_inv, scale, ((0, 0),), [mate], [own], [], n_form=1)
    later, acc = lax.optimization_barrier((field, acc))
    cross = toward(later, 3, -3)
    near, acc = lax.optimization_barrier((near, acc))
    accs = [acc]
    for hop in range(1, hops):
        here, there = near, cross
        near = toward(here, -2, 2)
        accs = visit(half_inv, scale, ((0, 1), (0, 0)), [here], [own, own_mate], accs)
        there, near_accs = lax.optimization_barrier((there, accs))
        cross = toward(there, -2, 2)
        accs = visit(half_inv, scale, ((0, 1), (0, 0)), [there], [own, own_mate], near_accs)
    (acc,) = visit(half_inv, scale, ((0, 0),), [near], [own_mate], accs[1:])
    cross, acc = lax.optimization_barrier((cross, acc))
    _, theirs = visit(half_inv, scale, ((0, 0),), [cross], [own_mate], [acc], done=(0,), fields=[mate])
    theirs = swapped(theirs)
    _, mine = visit(half_inv, scale, ((0, 0),), [near], [own], accs[:1], done=(0,), fields=[field])
    total = mine + theirs
    return (-(root_five / 3.0) / lengthscale)[:, None] * total


def solution(mesh):
    return jax.shard_map(
        on_device,
        mesh=mesh,
        in_specs=(
            P(None, ("groups", "blk")),
            P(("groups", "blk")),
            P(None, ("groups", "blk")),
            P(None, ("groups", "blk")),
            P(),
        ),
        out_specs=P(None, ("groups", "blk")),
        check_vma=False,
    )
```

```python
import functools

import jax
import jax.numpy as jnp
from jax import lax
from jax.experimental import pallas as pl
from jax.experimental.pallas import tpu as pltpu
from jax.sharding import PartitionSpec as P

root_five = 5.0**0.5
minus_log2e = -1.4426950408889634
f32, bf16 = jnp.float32, jnp.bfloat16
VMEM = pl.BlockSpec(memory_space=pltpu.VMEM)
DIM, GROUP, SUMS = 32, 16, 80
STEP, BACK, AHEAD, LAG = 192, 192, 1, 1


def halves(value):
    high = value.astype(bf16)
    return high, (value - high.astype(f32)).astype(bf16)


def row_is(row, value, other):
    return jnp.where(lax.broadcasted_iota(jnp.int32, other.shape, 0) == row, value, other)


def edge_rows(square, parts_at, ones_at):
    one = square.astype(bf16).astype(f32)
    rest = square - one
    two = rest.astype(bf16).astype(f32)
    row = lax.broadcasted_iota(jnp.int32, square.shape, 0)
    edge = jnp.where((row >= ones_at) & (row < ones_at + 3), 1.0, 0.0)
    for index, part in enumerate((one, two, rest - two)):
        edge = row_is(parts_at + index, part, edge)
    return edge.astype(bf16)


def scaled_halves(field, scale):
    wide = jnp.concatenate([scale] * (field.shape[1] // scale.shape[1]), 1)
    high, low = halves((field[:DIM] - wide[DIM:]) * wide[:DIM])
    return high, low, high.astype(f32) + low.astype(f32)


def own_forms(field, scale, dist_ref, coup_ref):
    high, low, near = scaled_halves(field, scale)
    first, second = field[DIM : DIM + GROUP], field[DIM + GROUP :]
    square = jnp.broadcast_to(jnp.sum(near * near, 0, keepdims=True), first.shape)
    dist_ref[...] = jnp.concatenate([high, low, high, low, edge_rows(square, 3, 0)], 0)
    table = jnp.concatenate([row_is(0, first, second), row_is(0, 0.0, first)], 0)
    high, low = halves(table)
    coup_ref[...] = jnp.concatenate([high, low, high, low], 0)


def visit_forms(half_inv, field, scale, dist_ref, coup_ref, sums_ref):
    points = field.shape[1]
    high, low, near = scaled_halves(field, scale)
    first, second = field[DIM : DIM + GROUP], field[DIM + GROUP :]
    sums_ref[...] = jnp.concatenate([high, low, jnp.ones((GROUP, points), bf16)], 0)
    square = jnp.broadcast_to(jnp.sum(near * near, 0, keepdims=True), first.shape)
    twice = [-2.0 * high, -2.0 * low]
    zero = jnp.zeros((256 - 4 * DIM - GROUP, points), bf16)
    dist = jnp.concatenate([*twice, *twice[::-1], edge_rows(square, 0, 3), zero], 0)
    dist_ref[...] = dist.T
    table = jnp.concatenate(
        [row_is(0, first, -half_inv * first), row_is(0, 0.0, -half_inv * second)], 0
    )
    high, low = halves(table)
    coup_ref[...] = jnp.concatenate([high, high, low, low], 0).T


def weights(dist, coup):
    dist = jnp.maximum(dist, 1e-30)
    scaled = dist * lax.rsqrt(dist)
    return coup * ((1.0 + scaled) * jnp.exp2(scaled * minus_log2e))


def dot(left, right):
    return lax.dot_general(
        left, right, (((1,), (0,)), ((), ())), preferred_element_type=f32
    )


def add_tiles(pairs, sides, own, accs, high_ref, low_ref):
    points = accs[0].shape[1]
    width = high_ref.shape[2]
    depth = own[0][0].shape[0]
    chunks = [
        (v, o, start, begin)
        for v, o in pairs
        for start in range(0, points, width)
        for begin in range(0, points, STEP)
    ]

    def front(chunk):
        v, o, start, begin = chunk
        rows, cols = slice(begin, begin + STEP), slice(start, start + width)
        return (
            dot(sides[v][0][rows, :depth], own[o][0][:, cols]),
            dot(sides[v][1][rows, :], own[o][1][:, cols]),
        )

    def middle(chunk, products, slot):
        v, o, start, begin = chunk
        rows = slice(begin, begin + STEP)
        high, low = halves(weights(*products))
        high_ref[slot, rows, :] = high
        low_ref[slot, rows, :] = low

    def back(chunk, slot):
        v, o, start, begin = chunk
        sums = sides[v][2][:, begin : begin + BACK]
        rows, cols = slice(begin, begin + BACK), slice(start, start + width)
        accs[o][:, cols] += dot(sums, high_ref[slot, rows, :]) + dot(sums, low_ref[slot, rows, :])

    per = points // STEP
    slot_of = lambda index: (index // per) % 2
    per_back = BACK // STEP
    products = {}
    for index in range(min(AHEAD, len(chunks))):
        products[index] = front(chunks[index])
    for index, chunk in enumerate(chunks):
        if index + AHEAD < len(chunks):
            products[index + AHEAD] = front(chunks[index + AHEAD])
        middle(chunk, products.pop(index), slot_of(index))
        late = index - LAG
        if late >= 0 and late % per_back == per_back - 1:
            first = late - per_back + 1
            back(chunks[first], slot_of(first))
    for late in range(len(chunks) - LAG, len(chunks)):
        if late % per_back == per_back - 1:
            first = late - per_back + 1
            back(chunks[first], slot_of(first))


def finish(field, scale, acc):
    near = scaled_halves(field, scale)[2]
    return near * acc[2 * DIM : 2 * DIM + 1] - (acc[:DIM] + acc[DIM : 2 * DIM])


def visit_kernel(half_inv, pairs, n_vis, n_own, n_acc, n_form, done, *refs):
    refs = list(refs)

    def take(count):
        taken, refs[:] = refs[:count], refs[count:]
        return taken

    (scale,) = take(1)
    vis = take(n_vis)
    own = [take(2) for _ in range(n_own)]
    acc_in = take(n_acc)
    fields = take(len(done))
    acc_out = take(n_own)
    forms = [take(2) for _ in range(n_form)]
    outs = take(len(done))
    high_ref, low_ref = take(2)
    for index in range(n_own):
        if index < n_acc:
            acc_out[index][...] = acc_in[index][...]
        else:
            acc_out[index][...] = jnp.zeros_like(acc_out[index])
    for index in range(n_form):
        own_forms(vis[index][...], scale[...], *forms[index])
    sides = []
    for ref in vis:
        side = take(3)
        visit_forms(half_inv, ref[...], scale[...], *side)
        sides.append(side)
    add_tiles(pairs, sides, own, acc_out, high_ref, low_ref)
    for o, field, out in zip(done, fields, outs):
        out[...] = finish(field[...], scale[...], acc_out[o][...])


def visit(half_inv, scale, pairs, vis, own, accs, n_form=0, done=(), fields=()):
    points = vis[0].shape[1]
    n_own = len(own)
    acc_shape = jax.ShapeDtypeStruct((SUMS, points), f32)
    form_shapes = [
        jax.ShapeDtypeStruct((4 * DIM + GROUP, points), bf16),
        jax.ShapeDtypeStruct((8 * GROUP, points), bf16),
    ]
    out_shape = [acc_shape] * n_own + form_shapes * n_form
    out_shape += [jax.ShapeDtypeStruct((DIM, points), f32)] * len(done)
    scratch = [pltpu.VMEM((2, points, 256), bf16)] * 2
    for _ in vis:
        scratch += [
            pltpu.VMEM((points, 256), bf16),
            pltpu.VMEM((points, 8 * GROUP), bf16),
            pltpu.VMEM((SUMS, points), bf16),
        ]
    args = [scale, *vis, *[ref for forms in own for ref in forms], *accs, *fields]
    first = 1 + len(vis) + 2 * n_own
    return pl.pallas_call(
        functools.partial(
            visit_kernel, half_inv, pairs, len(vis), n_own, len(accs), n_form, done
        ),
        out_shape=out_shape,
        in_specs=[VMEM] * len(args),
        out_specs=[VMEM] * len(out_shape),
        scratch_shapes=scratch,
        input_output_aliases={first + index: index for index in range(len(accs))},
        compiler_params=pltpu.CompilerParams(vmem_limit_bytes=20 * 2**20),
        cost_estimate=pl.CostEstimate(
            flops=len(pairs) * 10**9, bytes_accessed=10**6, transcendentals=0
        ),
        name="visit",
    )(*args)


def field_kernel(coords, alpha, solves, probes, field):
    middle = DIM + GROUP
    lanes = alpha.shape[1]
    field[0:DIM, :] = coords[...]
    for index in range(alpha.shape[0]):
        cols = slice(index * lanes, (index + 1) * lanes)
        field[DIM : DIM + 1, cols] = alpha[index : index + 1, :]
        field[middle : middle + 1, cols] = alpha[index : index + 1, :]
    field[DIM + 1 : middle, :] = solves[...]
    field[middle + 1 :, :] = probes[...]


def make_field(coords, alpha, solves, probes):
    args = (coords * root_five, alpha.reshape(-1, 128), solves, probes)
    return pl.pallas_call(
        field_kernel,
        out_shape=jax.ShapeDtypeStruct((DIM + 2 * GROUP, coords.shape[1]), f32),
        in_specs=[VMEM] * len(args),
        out_specs=VMEM,
        compiler_params=pltpu.CompilerParams(vmem_limit_bytes=8 * 2**20),
        name="field",
    )(*args)


def scale_kernel(field, length, scale_ref, dist_ref, coup_ref):
    size = length.shape[1]
    spread = jnp.broadcast_to(length[...], (size, size))
    row = lax.broadcasted_iota(jnp.int32, (size, size), 0)
    col = lax.broadcasted_iota(jnp.int32, (size, size), 1)
    column = jnp.sum(jnp.where(row == col, spread, 0.0), 1, keepdims=True)
    centre = jnp.mean(field[:DIM, :], 1, keepdims=True)
    scale = jnp.concatenate(
        [jnp.broadcast_to(part, (DIM, scale_ref.shape[1])) for part in (1.0 / column, centre)], 0
    )
    scale_ref[...] = scale
    own_forms(field[...], scale, dist_ref, coup_ref)


def make_own(field, lengthscale):
    points = field.shape[1]
    return pl.pallas_call(
        scale_kernel,
        out_shape=[
            jax.ShapeDtypeStruct((2 * DIM, 128), f32),
            jax.ShapeDtypeStruct((4 * DIM + GROUP, points), bf16),
            jax.ShapeDtypeStruct((8 * GROUP, points), bf16),
        ],
        in_specs=[VMEM] * 2,
        out_specs=[VMEM] * 3,
        compiler_params=pltpu.CompilerParams(vmem_limit_bytes=8 * 2**20),
        name="own",
    )(field, lengthscale[None])


def swapped(value):
    count = lax.axis_size("blk")
    return lax.ppermute(value, "blk", [(b, b + 1 - 2 * (b % 2)) for b in range(count)])


def toward(value, even, odd):
    count = lax.axis_size("blk")
    pairs = [(b, (b + (odd if b % 2 else even)) % count) for b in range(count)]
    return lax.ppermute(value, "blk", pairs)


def on_device(coords, alpha, probe_solves, probes, lengthscale):
    half_inv = 1.0 / (2.0 * probes.shape[0])
    hops = lax.axis_size("blk") // 8
    field = make_field(coords, alpha, probe_solves, probes)
    mate = swapped(field)
    near = toward(field, -2, 2)
    scale, *own = make_own(field, lengthscale)
    mate, own = lax.optimization_barrier((mate, own))
    acc, *own_mate = visit(half_inv, scale, ((0, 0),), [mate], [own], [], n_form=1)
    later, acc = lax.optimization_barrier((field, acc))
    cross = toward(later, 3, -3)
    near, acc = lax.optimization_barrier((near, acc))
    accs = [acc]
    for hop in range(1, hops):
        here, there = near, cross
        near = toward(here, -2, 2)
        accs = visit(half_inv, scale, ((0, 1), (0, 0)), [here], [own, own_mate], accs)
        there, near_accs = lax.optimization_barrier((there, accs))
        cross = toward(there, -2, 2)
        accs = visit(half_inv, scale, ((0, 1), (0, 0)), [there], [own, own_mate], near_accs)
    (acc,) = visit(half_inv, scale, ((0, 0),), [near], [own_mate], accs[1:])
    cross, acc = lax.optimization_barrier((cross, acc))
    _, theirs = visit(half_inv, scale, ((0, 0),), [cross], [own_mate], [acc], done=(0,), fields=[mate])
    theirs = swapped(theirs)
    _, mine = visit(half_inv, scale, ((0, 0),), [near], [own], accs[:1], done=(0,), fields=[field])
    total = mine + theirs
    return (-(root_five / 3.0) / lengthscale)[:, None] * total


def solution(mesh):
    return jax.shard_map(
        on_device,
        mesh=mesh,
        in_specs=(
            P(None, ("groups", "blk")),
            P(("groups", "blk")),
            P(None, ("groups", "blk")),
            P(None, ("groups", "blk")),
            P(),
        ),
        out_specs=P(None, ("groups", "blk")),
        check_vma=False,
    )
```

```python
import functools

import jax
import jax.numpy as jnp
from jax import lax
from jax.experimental import pallas as pl
from jax.experimental.pallas import tpu as pltpu
from jax.sharding import PartitionSpec as P

root_five = 5.0**0.5
minus_log2e = -1.4426950408889634
f32, bf16 = jnp.float32, jnp.bfloat16
VMEM = pl.BlockSpec(memory_space=pltpu.VMEM)
DIM, GROUP, SUMS = 32, 16, 80
STEP, BACK, AHEAD, LAG = 192, 192, 1, 1


def halves(value):
    high = value.astype(bf16)
    return high, (value - high.astype(f32)).astype(bf16)


def row_is(row, value, other):
    return jnp.where(lax.broadcasted_iota(jnp.int32, other.shape, 0) == row, value, other)


def edge_rows(square, parts_at, ones_at):
    one = square.astype(bf16).astype(f32)
    rest = square - one
    two = rest.astype(bf16).astype(f32)
    row = lax.broadcasted_iota(jnp.int32, square.shape, 0)
    edge = jnp.where((row >= ones_at) & (row < ones_at + 3), 1.0, 0.0)
    for index, part in enumerate((one, two, rest - two)):
        edge = row_is(parts_at + index, part, edge)
    return edge.astype(bf16)


def scaled_halves(field, scale):
    wide = jnp.concatenate([scale] * (field.shape[1] // scale.shape[1]), 1)
    high, low = halves((field[:DIM] - wide[DIM:]) * wide[:DIM])
    return high, low, high.astype(f32) + low.astype(f32)


def own_forms(field, scale, dist_ref, coup_ref):
    high, low, near = scaled_halves(field, scale)
    first, second = field[DIM : DIM + GROUP], field[DIM + GROUP :]
    square = jnp.broadcast_to(jnp.sum(near * near, 0, keepdims=True), first.shape)
    dist_ref[...] = jnp.concatenate([high, low, high, low, edge_rows(square, 3, 0)], 0)
    table = jnp.concatenate([row_is(0, first, second), row_is(0, 0.0, first)], 0)
    high, low = halves(table)
    coup_ref[...] = jnp.concatenate([high, low, high, low], 0)


def visit_forms(half_inv, field, scale, dist_ref, coup_ref, sums_ref):
    points = field.shape[1]
    high, low, near = scaled_halves(field, scale)
    first, second = field[DIM : DIM + GROUP], field[DIM + GROUP :]
    sums = jnp.concatenate([high, low, jnp.ones((GROUP, points), bf16)], 0)
    for index in range(points // BACK):
        sums_ref[index] = sums[:, index * BACK : (index + 1) * BACK]
    square = jnp.broadcast_to(jnp.sum(near * near, 0, keepdims=True), first.shape)
    twice = [-2.0 * high, -2.0 * low]
    zero = jnp.zeros((256 - 4 * DIM - GROUP, points), bf16)
    dist = jnp.concatenate([*twice, *twice[::-1], edge_rows(square, 0, 3), zero], 0)
    dist_ref[...] = dist.T
    table = jnp.concatenate(
        [row_is(0, first, -half_inv * first), row_is(0, 0.0, -half_inv * second)], 0
    )
    high, low = halves(table)
    coup_ref[...] = jnp.concatenate([high, high, low, low], 0).T


def weights(dist, coup):
    dist = jnp.maximum(dist, 1e-30)
    scaled = dist * lax.rsqrt(dist)
    return coup * ((1.0 + scaled) * jnp.exp2(scaled * minus_log2e))


def dot(left, right):
    return lax.dot_general(
        left, right, (((1,), (0,)), ((), ())), preferred_element_type=f32
    )


def add_tiles(pairs, sides, own, accs, high_ref, low_ref):
    points = accs[0].shape[1]
    width = high_ref.shape[2]
    depth = own[0][0].shape[0]
    chunks = [
        (v, o, start, begin)
        for v, o in pairs
        for start in range(0, points, width)
        for begin in range(0, points, STEP)
    ]

    def front(chunk):
        v, o, start, begin = chunk
        rows, cols = slice(begin, begin + STEP), slice(start, start + width)
        return (
            dot(sides[v][0][rows, :depth], own[o][0][:, cols]),
            dot(sides[v][1][rows, :], own[o][1][:, cols]),
        )

    def middle(chunk, products, slot):
        v, o, start, begin = chunk
        rows = slice(begin, begin + STEP)
        high, low = halves(weights(*products))
        high_ref[slot, rows, :] = high
        low_ref[slot, rows, :] = low

    def back(chunk, slot):
        v, o, start, begin = chunk
        sums = sides[v][2][begin // BACK]
        rows, cols = slice(begin, begin + BACK), slice(start, start + width)
        accs[o][:, cols] += dot(sums, high_ref[slot, rows, :]) + dot(sums, low_ref[slot, rows, :])

    per = points // STEP
    slot_of = lambda index: (index // per) % 2
    per_back = BACK // STEP
    products = {}
    for index in range(min(AHEAD, len(chunks))):
        products[index] = front(chunks[index])
    for index, chunk in enumerate(chunks):
        if index + AHEAD < len(chunks):
            products[index + AHEAD] = front(chunks[index + AHEAD])
        middle(chunk, products.pop(index), slot_of(index))
        late = index - LAG
        if late >= 0 and late % per_back == per_back - 1:
            first = late - per_back + 1
            back(chunks[first], slot_of(first))
    for late in range(len(chunks) - LAG, len(chunks)):
        if late % per_back == per_back - 1:
            first = late - per_back + 1
            back(chunks[first], slot_of(first))


def finish(field, scale, acc):
    near = scaled_halves(field, scale)[2]
    return near * acc[2 * DIM : 2 * DIM + 1] - (acc[:DIM] + acc[DIM : 2 * DIM])


def visit_kernel(half_inv, pairs, n_vis, n_own, n_acc, n_form, done, *refs):
    refs = list(refs)

    def take(count):
        taken, refs[:] = refs[:count], refs[count:]
        return taken

    (scale,) = take(1)
    vis = take(n_vis)
    own = [take(2) for _ in range(n_own)]
    acc_in = take(n_acc)
    fields = take(len(done))
    acc_out = take(n_own)
    forms = [take(2) for _ in range(n_form)]
    outs = take(len(done))
    high_ref, low_ref = take(2)
    for index in range(n_own):
        if index < n_acc:
            acc_out[index][...] = acc_in[index][...]
        else:
            acc_out[index][...] = jnp.zeros_like(acc_out[index])
    for index in range(n_form):
        own_forms(vis[index][...], scale[...], *forms[index])
    sides = []
    for ref in vis:
        side = take(3)
        visit_forms(half_inv, ref[...], scale[...], *side)
        sides.append(side)
    add_tiles(pairs, sides, own, acc_out, high_ref, low_ref)
    for o, field, out in zip(done, fields, outs):
        out[...] = finish(field[...], scale[...], acc_out[o][...])


def visit(half_inv, scale, pairs, vis, own, accs, n_form=0, done=(), fields=()):
    points = vis[0].shape[1]
    n_own = len(own)
    acc_shape = jax.ShapeDtypeStruct((SUMS, points), f32)
    form_shapes = [
        jax.ShapeDtypeStruct((4 * DIM + GROUP, points), bf16),
        jax.ShapeDtypeStruct((8 * GROUP, points), bf16),
    ]
    out_shape = [acc_shape] * n_own + form_shapes * n_form
    out_shape += [jax.ShapeDtypeStruct((DIM, points), f32)] * len(done)
    scratch = [pltpu.VMEM((2, points, 256), bf16)] * 2
    for _ in vis:
        scratch += [
            pltpu.VMEM((points, 256), bf16),
            pltpu.VMEM((points, 8 * GROUP), bf16),
            pltpu.VMEM((points // BACK, SUMS, BACK), bf16),
        ]
    args = [scale, *vis, *[ref for forms in own for ref in forms], *accs, *fields]
    first = 1 + len(vis) + 2 * n_own
    return pl.pallas_call(
        functools.partial(
            visit_kernel, half_inv, pairs, len(vis), n_own, len(accs), n_form, done
        ),
        out_shape=out_shape,
        in_specs=[VMEM] * len(args),
        out_specs=[VMEM] * len(out_shape),
        scratch_shapes=scratch,
        input_output_aliases={first + index: index for index in range(len(accs))},
        compiler_params=pltpu.CompilerParams(vmem_limit_bytes=20 * 2**20),
        cost_estimate=pl.CostEstimate(
            flops=len(pairs) * 10**9, bytes_accessed=10**6, transcendentals=0
        ),
        name="visit",
    )(*args)


def field_kernel(coords, alpha, solves, probes, field):
    middle = DIM + GROUP
    lanes = alpha.shape[1]
    field[0:DIM, :] = coords[...]
    for index in range(alpha.shape[0]):
        cols = slice(index * lanes, (index + 1) * lanes)
        field[DIM : DIM + 1, cols] = alpha[index : index + 1, :]
        field[middle : middle + 1, cols] = alpha[index : index + 1, :]
    field[DIM + 1 : middle, :] = solves[...]
    field[middle + 1 :, :] = probes[...]


def make_field(coords, alpha, solves, probes):
    args = (coords * root_five, alpha.reshape(-1, 128), solves, probes)
    return pl.pallas_call(
        field_kernel,
        out_shape=jax.ShapeDtypeStruct((DIM + 2 * GROUP, coords.shape[1]), f32),
        in_specs=[VMEM] * len(args),
        out_specs=VMEM,
        compiler_params=pltpu.CompilerParams(vmem_limit_bytes=8 * 2**20),
        name="field",
    )(*args)


def scale_kernel(field, length, scale_ref, dist_ref, coup_ref):
    size = length.shape[1]
    spread = jnp.broadcast_to(length[...], (size, size))
    row = lax.broadcasted_iota(jnp.int32, (size, size), 0)
    col = lax.broadcasted_iota(jnp.int32, (size, size), 1)
    column = jnp.sum(jnp.where(row == col, spread, 0.0), 1, keepdims=True)
    centre = jnp.mean(field[:DIM, :], 1, keepdims=True)
    scale = jnp.concatenate(
        [jnp.broadcast_to(part, (DIM, scale_ref.shape[1])) for part in (1.0 / column, centre)], 0
    )
    scale_ref[...] = scale
    own_forms(field[...], scale, dist_ref, coup_ref)


def make_own(field, lengthscale):
    points = field.shape[1]
    return pl.pallas_call(
        scale_kernel,
        out_shape=[
            jax.ShapeDtypeStruct((2 * DIM, 128), f32),
            jax.ShapeDtypeStruct((4 * DIM + GROUP, points), bf16),
            jax.ShapeDtypeStruct((8 * GROUP, points), bf16),
        ],
        in_specs=[VMEM] * 2,
        out_specs=[VMEM] * 3,
        compiler_params=pltpu.CompilerParams(vmem_limit_bytes=8 * 2**20),
        name="own",
    )(field, lengthscale[None])


def swapped(value):
    count = lax.axis_size("blk")
    return lax.ppermute(value, "blk", [(b, b + 1 - 2 * (b % 2)) for b in range(count)])


def toward(value, even, odd):
    count = lax.axis_size("blk")
    pairs = [(b, (b + (odd if b % 2 else even)) % count) for b in range(count)]
    return lax.ppermute(value, "blk", pairs)


def on_device(coords, alpha, probe_solves, probes, lengthscale):
    half_inv = 1.0 / (2.0 * probes.shape[0])
    hops = lax.axis_size("blk") // 8
    field = make_field(coords, alpha, probe_solves, probes)
    mate = swapped(field)
    near = toward(field, -2, 2)
    scale, *own = make_own(field, lengthscale)
    mate, own = lax.optimization_barrier((mate, own))
    acc, *own_mate = visit(half_inv, scale, ((0, 0),), [mate], [own], [], n_form=1)
    later, acc = lax.optimization_barrier((field, acc))
    cross = toward(later, 3, -3)
    near, acc = lax.optimization_barrier((near, acc))
    accs = [acc]
    for hop in range(1, hops):
        here, there = near, cross
        near = toward(here, -2, 2)
        accs = visit(half_inv, scale, ((0, 1), (0, 0)), [here], [own, own_mate], accs)
        there, near_accs = lax.optimization_barrier((there, accs))
        cross = toward(there, -2, 2)
        accs = visit(half_inv, scale, ((0, 1), (0, 0)), [there], [own, own_mate], near_accs)
    (acc,) = visit(half_inv, scale, ((0, 0),), [near], [own_mate], accs[1:])
    cross, acc = lax.optimization_barrier((cross, acc))
    _, theirs = visit(half_inv, scale, ((0, 0),), [cross], [own_mate], [acc], done=(0,), fields=[mate])
    theirs = swapped(theirs)
    _, mine = visit(half_inv, scale, ((0, 0),), [near], [own], accs[:1], done=(0,), fields=[field])
    total = mine + theirs
    return (-(root_five / 3.0) / lengthscale)[:, None] * total


def solution(mesh):
    return jax.shard_map(
        on_device,
        mesh=mesh,
        in_specs=(
            P(None, ("groups", "blk")),
            P(("groups", "blk")),
            P(None, ("groups", "blk")),
            P(None, ("groups", "blk")),
            P(),
        ),
        out_specs=P(None, ("groups", "blk")),
        check_vma=False,
    )
```

```python
import functools

import jax
import jax.numpy as jnp
from jax import lax
from jax.experimental import pallas as pl
from jax.experimental.pallas import tpu as pltpu
from jax.sharding import PartitionSpec as P

root_five = 5.0**0.5
minus_log2e = -1.4426950408889634
f32, bf16 = jnp.float32, jnp.bfloat16
VMEM = pl.BlockSpec(memory_space=pltpu.VMEM)
DIM, GROUP, SUMS = 32, 16, 80
STEP, BACK, AHEAD, LAG = 192, 192, 1, 1


def halves(value):
    high = value.astype(bf16)
    return high, (value - high.astype(f32)).astype(bf16)


def row_is(row, value, other):
    return jnp.where(lax.broadcasted_iota(jnp.int32, other.shape, 0) == row, value, other)


def edge_rows(square, parts_at, ones_at):
    one = square.astype(bf16).astype(f32)
    rest = square - one
    two = rest.astype(bf16).astype(f32)
    row = lax.broadcasted_iota(jnp.int32, square.shape, 0)
    edge = jnp.where((row >= ones_at) & (row < ones_at + 3), 1.0, 0.0)
    for index, part in enumerate((one, two, rest - two)):
        edge = row_is(parts_at + index, part, edge)
    return edge.astype(bf16)


def scaled_halves(field, scale):
    wide = jnp.concatenate([scale] * (field.shape[1] // scale.shape[1]), 1)
    high, low = halves((field[:DIM] - wide[DIM:]) * wide[:DIM])
    return high, low, high.astype(f32) + low.astype(f32)


def own_forms(field, scale, dist_ref, coup_ref):
    high, low, near = scaled_halves(field, scale)
    first, second = field[DIM : DIM + GROUP], field[DIM + GROUP :]
    square = jnp.broadcast_to(jnp.sum(near * near, 0, keepdims=True), first.shape)
    dist_ref[...] = jnp.concatenate([high, low, high, low, edge_rows(square, 3, 0)], 0)
    table = jnp.concatenate([row_is(0, first, second), row_is(0, 0.0, first)], 0)
    high, low = halves(table)
    coup_ref[...] = jnp.concatenate([high, low, high, low], 0)


def visit_forms(half_inv, field, scale, dist_ref, coup_ref, sums_ref):
    points = field.shape[1]
    high, low, near = scaled_halves(field, scale)
    first, second = field[DIM : DIM + GROUP], field[DIM + GROUP :]
    sums = jnp.concatenate([high, low, jnp.ones((GROUP, points), bf16)], 0)
    for index in range(points // BACK):
        sums_ref[index] = sums[:, index * BACK : (index + 1) * BACK]
    square = jnp.broadcast_to(jnp.sum(near * near, 0, keepdims=True), first.shape)
    twice = [-2.0 * high, -2.0 * low]
    zero = jnp.zeros((256 - 4 * DIM - GROUP, points), bf16)
    dist = jnp.concatenate([*twice, *twice[::-1], edge_rows(square, 0, 3), zero], 0)
    dist_ref[...] = dist.T
    table = jnp.concatenate(
        [row_is(0, first, -half_inv * first), row_is(0, 0.0, -half_inv * second)], 0
    )
    high, low = halves(table)
    coup_ref[...] = jnp.concatenate([high, high, low, low], 0).T


def weights(dist, coup):
    dist = jnp.maximum(dist, 1e-30)
    scaled = dist * lax.rsqrt(dist)
    return coup * ((1.0 + scaled) * jnp.exp2(scaled * minus_log2e))


def dot(left, right):
    return lax.dot_general(
        left, right, (((1,), (0,)), ((), ())), preferred_element_type=f32
    )


def add_tiles(pairs, sides, own, accs, high_ref, low_ref):
    points = accs[0].shape[1]
    width = high_ref.shape[2]
    depth = own[0][0].shape[0]
    chunks = [
        (v, o, start, begin)
        for v, o in pairs
        for start in range(0, points, width)
        for begin in range(0, points, STEP)
    ]

    def front(chunk):
        v, o, start, begin = chunk
        rows, cols = slice(begin, begin + STEP), slice(start, start + width)
        return (
            dot(sides[v][0][rows, :depth], own[o][0][:, cols]),
            dot(sides[v][1][rows, :], own[o][1][:, cols]),
        )

    def middle(chunk, products, slot):
        v, o, start, begin = chunk
        rows = slice(begin, begin + STEP)
        high, low = halves(weights(*products))
        high_ref[slot, rows, :] = high
        low_ref[slot, rows, :] = low

    def back(chunk, slot):
        v, o, start, begin = chunk
        sums = sides[v][2][begin // BACK]
        rows, cols = slice(begin, begin + BACK), slice(start, start + width)
        accs[o][:, cols] += dot(sums, high_ref[slot, rows, :]) + dot(sums, low_ref[slot, rows, :])

    per = points // STEP
    slot_of = lambda index: (index // per) % 2
    per_back = BACK // STEP
    products = {}
    for index in range(min(AHEAD, len(chunks))):
        products[index] = front(chunks[index])
    for index, chunk in enumerate(chunks):
        if index + AHEAD < len(chunks):
            products[index + AHEAD] = front(chunks[index + AHEAD])
        middle(chunk, products.pop(index), slot_of(index))
        late = index - LAG
        if late >= 0 and late % per_back == per_back - 1:
            first = late - per_back + 1
            back(chunks[first], slot_of(first))
    for late in range(len(chunks) - LAG, len(chunks)):
        if late % per_back == per_back - 1:
            first = late - per_back + 1
            back(chunks[first], slot_of(first))


def finish(field, scale, acc):
    near = scaled_halves(field, scale)[2]
    return near * acc[2 * DIM : 2 * DIM + 1] - (acc[:DIM] + acc[DIM : 2 * DIM])


def visit_kernel(half_inv, pairs, n_vis, n_own, n_acc, n_form, done, *refs):
    refs = list(refs)

    def take(count):
        taken, refs[:] = refs[:count], refs[count:]
        return taken

    (scale,) = take(1)
    vis = take(n_vis)
    own = [take(2) for _ in range(n_own)]
    acc_in = take(n_acc)
    fields = take(len(done))
    acc_out = take(n_own)
    forms = [take(2) for _ in range(n_form)]
    outs = take(len(done))
    high_ref, low_ref = take(2)
    for index in range(n_own):
        if index < n_acc:
            acc_out[index][...] = acc_in[index][...]
        else:
            acc_out[index][...] = jnp.zeros_like(acc_out[index])
    for index in range(n_form):
        own_forms(vis[index][...], scale[...], *forms[index])
    sides = []
    for ref in vis:
        side = take(3)
        visit_forms(half_inv, ref[...], scale[...], *side)
        sides.append(side)
    add_tiles(pairs, sides, own, acc_out, high_ref, low_ref)
    for o, field, out in zip(done, fields, outs):
        out[...] = finish(field[...], scale[...], acc_out[o][...])


def visit(half_inv, scale, pairs, vis, own, accs, n_form=0, done=(), fields=()):
    points = vis[0].shape[1]
    n_own = len(own)
    acc_shape = jax.ShapeDtypeStruct((SUMS, points), f32)
    form_shapes = [
        jax.ShapeDtypeStruct((4 * DIM + GROUP, points), bf16),
        jax.ShapeDtypeStruct((8 * GROUP, points), bf16),
    ]
    out_shape = [acc_shape] * n_own + form_shapes * n_form
    out_shape += [jax.ShapeDtypeStruct((DIM, points), f32)] * len(done)
    scratch = [pltpu.VMEM((2, points, 256), bf16)] * 2
    for _ in vis:
        scratch += [
            pltpu.VMEM((points, 256), bf16),
            pltpu.VMEM((points, 8 * GROUP), bf16),
            pltpu.VMEM((points // BACK, SUMS, BACK), bf16),
        ]
    args = [scale, *vis, *[ref for forms in own for ref in forms], *accs, *fields]
    first = 1 + len(vis) + 2 * n_own
    return pl.pallas_call(
        functools.partial(
            visit_kernel, half_inv, pairs, len(vis), n_own, len(accs), n_form, done
        ),
        out_shape=out_shape,
        in_specs=[VMEM] * len(args),
        out_specs=[VMEM] * len(out_shape),
        scratch_shapes=scratch,
        input_output_aliases={first + index: index for index in range(len(accs))},
        compiler_params=pltpu.CompilerParams(vmem_limit_bytes=20 * 2**20),
        cost_estimate=pl.CostEstimate(
            flops=2 * 10**9, bytes_accessed=10**6, transcendentals=0
        ),
        name="visit",
    )(*args)


def field_kernel(coords, alpha, solves, probes, field):
    middle = DIM + GROUP
    lanes = alpha.shape[1]
    field[0:DIM, :] = coords[...]
    for index in range(alpha.shape[0]):
        cols = slice(index * lanes, (index + 1) * lanes)
        field[DIM : DIM + 1, cols] = alpha[index : index + 1, :]
        field[middle : middle + 1, cols] = alpha[index : index + 1, :]
    field[DIM + 1 : middle, :] = solves[...]
    field[middle + 1 :, :] = probes[...]


def make_field(coords, alpha, solves, probes):
    args = (coords * root_five, alpha.reshape(-1, 128), solves, probes)
    return pl.pallas_call(
        field_kernel,
        out_shape=jax.ShapeDtypeStruct((DIM + 2 * GROUP, coords.shape[1]), f32),
        in_specs=[VMEM] * len(args),
        out_specs=VMEM,
        compiler_params=pltpu.CompilerParams(vmem_limit_bytes=8 * 2**20),
        name="field",
    )(*args)


def scale_kernel(field, length, scale_ref, dist_ref, coup_ref):
    size = length.shape[1]
    spread = jnp.broadcast_to(length[...], (size, size))
    row = lax.broadcasted_iota(jnp.int32, (size, size), 0)
    col = lax.broadcasted_iota(jnp.int32, (size, size), 1)
    column = jnp.sum(jnp.where(row == col, spread, 0.0), 1, keepdims=True)
    centre = jnp.mean(field[:DIM, :], 1, keepdims=True)
    scale = jnp.concatenate(
        [jnp.broadcast_to(part, (DIM, scale_ref.shape[1])) for part in (1.0 / column, centre)], 0
    )
    scale_ref[...] = scale
    own_forms(field[...], scale, dist_ref, coup_ref)


def make_own(field, lengthscale):
    points = field.shape[1]
    return pl.pallas_call(
        scale_kernel,
        out_shape=[
            jax.ShapeDtypeStruct((2 * DIM, 128), f32),
            jax.ShapeDtypeStruct((4 * DIM + GROUP, points), bf16),
            jax.ShapeDtypeStruct((8 * GROUP, points), bf16),
        ],
        in_specs=[VMEM] * 2,
        out_specs=[VMEM] * 3,
        compiler_params=pltpu.CompilerParams(vmem_limit_bytes=8 * 2**20),
        name="own",
    )(field, lengthscale[None])


def swapped(value):
    count = lax.axis_size("blk")
    return lax.ppermute(value, "blk", [(b, b + 1 - 2 * (b % 2)) for b in range(count)])


def toward(value, even, odd):
    count = lax.axis_size("blk")
    pairs = [(b, (b + (odd if b % 2 else even)) % count) for b in range(count)]
    return lax.ppermute(value, "blk", pairs)


def on_device(coords, alpha, probe_solves, probes, lengthscale):
    half_inv = 1.0 / (2.0 * probes.shape[0])
    hops = lax.axis_size("blk") // 8
    field = make_field(coords, alpha, probe_solves, probes)
    mate = swapped(field)
    near = toward(field, -2, 2)
    scale, *own = make_own(field, lengthscale)
    mate, own = lax.optimization_barrier((mate, own))
    acc, *own_mate = visit(half_inv, scale, ((0, 0),), [mate], [own], [], n_form=1)
    later, acc = lax.optimization_barrier((field, acc))
    cross = toward(later, 3, -3)
    near, acc = lax.optimization_barrier((near, acc))
    accs = [acc]
    for hop in range(1, hops):
        here, there = near, cross
        near = toward(here, -2, 2)
        if hop < hops - 1:
            accs = visit(half_inv, scale, ((0, 1), (0, 0)), [here], [own, own_mate], accs)
        else:
            accs = accs[:1] + visit(half_inv, scale, ((0, 0),), [here], [own_mate], accs[1:])
        there, near_accs = lax.optimization_barrier((there, accs))
        cross = toward(there, -2, 2)
        accs = visit(half_inv, scale, ((0, 1), (0, 0)), [there], [own, own_mate], near_accs)
    accs = visit(half_inv, scale, ((0, 1), (1, 0)), [near, here], [own, own_mate], accs)
    cross, *accs = lax.optimization_barrier((cross, *accs))
    _, theirs = visit(half_inv, scale, ((0, 0),), [cross], [own_mate], accs[1:], done=(0,), fields=[mate])
    theirs = swapped(theirs)
    _, mine = visit(half_inv, scale, ((0, 0),), [near], [own], accs[:1], done=(0,), fields=[field])
    total = mine + theirs
    return (-(root_five / 3.0) / lengthscale)[:, None] * total


def solution(mesh):
    return jax.shard_map(
        on_device,
        mesh=mesh,
        in_specs=(
            P(None, ("groups", "blk")),
            P(("groups", "blk")),
            P(None, ("groups", "blk")),
            P(None, ("groups", "blk")),
            P(),
        ),
        out_specs=P(None, ("groups", "blk")),
        check_vma=False,
    )
```
